512 devices in a mesh: member: 2 (over y), slab: 32 (over z), chan: 4 (over x), mode: 2 (over core).
Axes of the slice: x: 4, y: 2, z: 32, core: 2. Of those that a mesh axis runs over, the one named last changes fastest.
The devices are a block of a 4x8x32 slice.
Arguments:
- source_field: float32 [128, 1024, 1024], P(('member', 'chan'), 'slab', 'mode'), parts along dimension 0, may hold values from -6 to 6
- cotangent: float32 [128, 1024, 1024], P(('member', 'chan'), 'slab', 'mode'), parts along dimension 0, may hold values from -6 to 6
- spectral_weight: float32 [128, 64, 32, 2, 64], P(('member', 'chan'), None, 'mode', None, 'slab'), parts along dimension 0, may hold values from -12 to 12
- skip_gain: float32 [128], P(('member', 'chan')), parts along dimension 0, may hold values from 0.5 to 2
- channel_bias: float32 [128], P(('member', 'chan')), parts along dimension 0, may hold values from -0.5 to 0.5
- mode_limit: int32 [128, 2], P('member'), parts along dimension 0, may hold values from 16 to 32
- width_limit: int32 [128], P('member'), parts along dimension 0, may hold values from 32 to 64
Outputs:
- output: float32 [128, 1024, 1024], P(('member', 'chan'), 'slab', 'mode'), parts along dimension 0
- field_grad: float32 [128, 1024, 1024], P(('member', 'chan'), 'slab', 'mode'), parts along dimension 0
- spectral_grad: float32 [128, 64, 32, 2, 64], P(('member', 'chan'), None, 'mode', None, 'slab'), parts along dimension 0
- gate_grad: float32 [128], P(('member', 'chan')), parts along dimension 0
- bias_grad: float32 [128], P(('member', 'chan')), parts along dimension 0
The draws below stay inside these ranges and needn't reach their ends.
There are 2 independent parts, one for each index of `member`. The reference program is written for one: setup_inputs(seed, part) draws one part's arguments, and reference() takes and returns one part's arrays. A program takes and returns all parts, laid end to end along the dimension named above; each array names one. Nothing has to cross between parts.
Inputs may be any that keep to these rules, and one draw needn't show every extreme that they name: `mode_limit`: never more than 32. `width_limit`: never more than 64.
All inputs are finite; a program needn't handle non-finite values.
Results may differ from the reference program's by a relative error of at most 0.00018.
Values sent between devices are 32-bit elements; how exact they have to be, the bound alone decides.
A program may use at most 64 MiB of HBM per device.

```python
import math
import jax
import jax.numpy as jnp
from jax import lax

C = 64
H = 1024
W = 1024
M = 32
KX = 64


def plant(values, stream_key, low, high):
    longest = values.shape.index(max(values.shape))
    spots = []
    for shift in (0, 1):
        where = [jax.random.randint(jax.random.fold_in(stream_key, axis), (), 0, length) for axis, length in enumerate(values.shape)]
        where[longest] = (where[longest] + shift) % values.shape[longest]
        spots.append(tuple(where))
    return values.at[spots[0]].set(low).at[spots[1]].set(high)


def levels(rng, shape, split, least, largest):
    factor_of = 1.0
    for dim, parts in split:
        steps = jax.random.uniform(jax.random.fold_in(jax.random.fold_in(rng, 6), dim), (parts,), jnp.float32, least / len(split), largest / len(split))
        factor_of = factor_of * jnp.repeat(jnp.exp(steps), shape[dim] // parts).reshape((-1,) + (1,) * (len(shape) - 1 - dim))
    return factor_of


def scatter_about(rng, dims, width, most, pieces=(), kind=jnp.bfloat16):
    entries = jax.random.normal(rng, dims, jnp.float32) * width
    if len(pieces) > 0:
        entries = levels(rng, dims, pieces, -0.22, 0.18) * entries
    return jnp.clip(entries, min=-most, max=most).astype(kind)


def setup_inputs(seed: int = 0, part: int = 0) -> dict:
    seeds = jax.random.split(jax.random.key(seed), 8)
    part_keys = jax.random.split(jax.random.fold_in(seeds[7], part), 8)
    return {
        "source_field": scatter_about(part_keys[0], (C, H, W), 1.0, 6.0, ((0, 4), (1, 32), (2, 2)), jnp.float32),
        "cotangent": scatter_about(part_keys[1], (C, H, W), 1.0, 6.0, ((0, 4), (1, 32), (2, 2)), jnp.float32),
        "spectral_weight": scatter_about(part_keys[2], (C, C, M, 2, KX), 2.0, 12.0, ((0, 4), (2, 2), (4, 32)), jnp.float32),
        "skip_gain": jnp.clip(jnp.exp(math.log(2.0) - 1.3862944 * jax.random.uniform(part_keys[3], (C,), jnp.float32) ** levels(part_keys[3], (C,), ((0, 4),), -0.2, 0.2)), 0.5, 2.0),
        "channel_bias": jnp.clip(jax.random.uniform(part_keys[4], (C,), jnp.float32, -0.5, 0.5) * levels(part_keys[4], (C,), ((0, 4),), -0.4, 0.0), -0.5, 0.5),
        "mode_limit": plant(jax.random.randint(part_keys[5], (C, 2), M // 2, M + 1), jax.random.fold_in(part_keys[5], 1), M // 2, M).astype(jnp.int32),
        "width_limit": plant(jax.random.randint(part_keys[6], (C,), C // 2, C + 1), jax.random.fold_in(part_keys[6], 1), C // 2, C).astype(jnp.int32),
    }


precise = lax.Precision.HIGHEST

def column_table(extent, freq_count, first_cell, cell_count):
    cell_index = first_cell + jnp.arange(cell_count, dtype=jnp.int32)
    wave_index = jnp.arange(freq_count, dtype=jnp.int32)
    products = (cell_index[:, None] * wave_index[None, :] % extent).astype(jnp.float32)
    angles = products * (2.0 * math.pi / extent)
    return jnp.stack([jnp.cos(angles), -jnp.sin(angles)], axis=-1).reshape(cell_count, 2 * freq_count)

def row_tables(extent, freq_count, first_cell, cell_count):
    cell_index = first_cell + jnp.arange(cell_count, dtype=jnp.int32)
    column = jnp.arange(2 * freq_count, dtype=jnp.int32)
    wave_index = (column + jnp.where(column >= freq_count, extent - 2 * freq_count, 0)).astype(jnp.int32)
    products = (cell_index[:, None] * wave_index[None, :] % extent).astype(jnp.float32)
    angles = products * (2.0 * math.pi / extent)
    return (jnp.cos(angles), jnp.sin(angles))

def spectrum(values, column_tab, row_cos, row_sin):
    channels, row_count, col_count = values.shape
    freq_count = column_tab.shape[1] // 2
    halves = jnp.einsum('chw,wk->chk', values, column_tab, precision=precise).reshape(channels, row_count, freq_count, 2)
    real_part = halves[..., 0]
    imag_part = halves[..., 1]
    out_real = jnp.einsum('chy,hx->cyx', real_part, row_cos, precision=precise) + jnp.einsum('chy,hx->cyx', imag_part, row_sin, precision=precise)
    out_imag = jnp.einsum('chy,hx->cyx', imag_part, row_cos, precision=precise) - jnp.einsum('chy,hx->cyx', real_part, row_sin, precision=precise)
    return jnp.stack([out_real, out_imag], axis=2)

def synthesis(modes_in, column_tab, row_cos, row_sin):
    channels = modes_in.shape[0]
    real_part = modes_in[:, :, 0]
    imag_part = modes_in[:, :, 1]
    back_real = jnp.einsum('cyx,hx->cyh', real_part, row_cos, precision=precise) - jnp.einsum('cyx,hx->cyh', imag_part, row_sin, precision=precise)
    back_imag = jnp.einsum('cyx,hx->cyh', real_part, row_sin, precision=precise) + jnp.einsum('cyx,hx->cyh', imag_part, row_cos, precision=precise)
    joined = jnp.stack([back_real, back_imag], axis=2).reshape(channels, -1, row_cos.shape[0])
    return jnp.einsum('ckh,wk->chw', joined, column_tab, precision=precise)

def contract(spectra, weight):
    spec_real = spectra[:, :, 0]
    spec_imag = spectra[:, :, 1]
    weight_real = weight[:, :, :, 0]
    weight_imag = weight[:, :, :, 1]
    out_real = jnp.einsum('iyx,ioyx->oyx', spec_real, weight_real, precision=precise) - jnp.einsum('iyx,ioyx->oyx', spec_imag, weight_imag, precision=precise)
    out_imag = jnp.einsum('iyx,ioyx->oyx', spec_real, weight_imag, precision=precise) + jnp.einsum('iyx,ioyx->oyx', spec_imag, weight_real, precision=precise)
    return jnp.stack([out_real, out_imag], axis=2)

def contract_back(grads, weight):
    grad_real = grads[:, :, 0]
    grad_imag = grads[:, :, 1]
    weight_real = weight[:, :, :, 0]
    weight_imag = weight[:, :, :, 1]
    back_real = jnp.einsum('oyx,ioyx->iyx', grad_real, weight_real, precision=precise) + jnp.einsum('oyx,ioyx->iyx', grad_imag, weight_imag, precision=precise)
    back_imag = jnp.einsum('oyx,ioyx->iyx', grad_imag, weight_real, precision=precise) - jnp.einsum('oyx,ioyx->iyx', grad_real, weight_imag, precision=precise)
    return jnp.stack([back_real, back_imag], axis=2)

def outer_grad(spectra, grads):
    spec_real = spectra[:, :, 0]
    spec_imag = spectra[:, :, 1]
    grad_real = grads[:, :, 0]
    grad_imag = grads[:, :, 1]
    real_side = jnp.einsum('iyx,oyx->ioyx', spec_real, grad_real) + jnp.einsum('iyx,oyx->ioyx', spec_imag, grad_imag)
    imag_side = jnp.einsum('iyx,oyx->ioyx', spec_real, grad_imag) - jnp.einsum('iyx,oyx->ioyx', spec_imag, grad_real)
    return jnp.stack([real_side, imag_side], axis=3)

def mode_weights(limit_rows, col_freq, row_freq, kx_count, cells_total):
    keep_cols = col_freq[None, :] < limit_rows[:, 0:1]
    keep_rows = (row_freq[None, :] < limit_rows[:, 1:2]) | ((kx_count - row_freq)[None, :] < limit_rows[:, 1:2])
    scales = jnp.where(col_freq == 0, 1.0, 2.0).astype(jnp.float32) / cells_total
    joined = keep_cols[:, :, None] & keep_rows[:, None, :]
    return (joined.astype(jnp.float32) * scales[None, :, None])[:, :, None, :]

def read_mask(in_index, width_limit):
    return (in_index[:, None] < width_limit[None, :]).astype(jnp.float32)[:, :, None, None, None]

def reference(source_field, cotangent, spectral_weight, skip_gain, channel_bias, mode_limit, width_limit):
    channels, row_count, col_count = source_field.shape
    freq_count = spectral_weight.shape[2]
    kx_count = spectral_weight.shape[4]
    column_tab = column_table(col_count, freq_count, 0, col_count)
    row_cos, row_sin = row_tables(row_count, freq_count, 0, row_count)
    weights = mode_weights(mode_limit, jnp.arange(freq_count, dtype=jnp.int32), jnp.arange(kx_count, dtype=jnp.int32), kx_count, row_count * col_count)
    reads = read_mask(jnp.arange(channels, dtype=jnp.int32), width_limit)
    masked_weight = spectral_weight * reads
    spectra = spectrum(source_field, column_tab, row_cos, row_sin)
    out_modes = contract(spectra, masked_weight) * weights
    branch = synthesis(out_modes, column_tab, row_cos, row_sin)
    skip_scale = skip_gain[:, None, None]
    summed = branch + skip_scale * source_field + channel_bias[:, None, None]
    output, gelu_back = jax.vjp(jax.nn.gelu, summed)
    grad_sum = gelu_back(cotangent)[0]
    grad_modes = spectrum(grad_sum, column_tab, row_cos, row_sin) * weights
    spectral_grad = outer_grad(spectra, grad_modes) * reads
    field_grad = synthesis(contract_back(grad_modes, masked_weight), column_tab, row_cos, row_sin) + skip_scale * grad_sum
    gate_grad = lax.optimization_barrier(jnp.sum(grad_sum * source_field, axis=(1, 2)))
    bias_grad = lax.optimization_barrier(jnp.sum(grad_sum, axis=(1, 2)))
    return (output, field_grad, spectral_grad, gate_grad, bias_grad)
```

```python
import functools
import math

import jax
import jax.numpy as jnp
from jax import lax
from jax.experimental import pallas as pl
from jax.experimental.pallas import tpu as pltpu
from jax.sharding import PartitionSpec as P

MESH = pl.DeviceIdType.MESH
LANES = 128
GELU_SLOPE = math.sqrt(2.0 / math.pi)
GELU_CUBE = 0.044715


def split(x):
    high = x.astype(jnp.bfloat16)
    low = (x - high.astype(jnp.float32)).astype(jnp.bfloat16)
    return high, low


def dot3(a, b):
    (ah, al), (bh, bl) = a, b
    dot = functools.partial(jnp.dot, preferred_element_type=jnp.float32)
    return dot(ah, bh) + (dot(ah, bl) + dot(al, bh))


def sine(turns, extent):
    half, quarter = extent // 2, extent // 4
    t = ((turns + half) & (extent - 1)) - half
    t = jnp.where(t > quarter, half - t, jnp.where(t < -quarter, -half - t, t))
    v = t.astype(jnp.float32) * (2.0 * math.pi / extent)
    s = v * v
    poly = -2.5052108e-8
    for c in (2.7557319e-6, -1.9841270e-4, 8.3333333e-3, -1.6666667e-1, 1.0):
        poly = poly * s + c
    return poly * v


def iota(shape, dim):
    return lax.broadcasted_iota(jnp.int32, shape, dim)


def kernel(
    dims,
    x_hbm, cot_hbm, w_hbm, gain, bias, limit, width,
    out_hbm, fgrad_hbm, sgrad_hbm, gate_ref, bgrad_ref,
    xv, cv, wv, gv, ov, tch, tcl, tth, ttl, fh, fl, fth, ftl,
    wt, zs, sv, sgv,
    own_cols, tx_cols, rx_cols, tx_rows, rx_rows, tx_chan, rx_chan, tile_tx, rx_modes,
    own_g, rx_g, g_chan, red_pair, red_all,
    lsem, osem, msend, mrecv, ssend, srecv, csend, crecv,
):
    slabs, chans, modes, rows, cols = dims
    chunk = 4 * rows
    me, ch, mo = lax.axis_index("slab"), lax.axis_index("chan"), lax.axis_index("mode")
    other = 1 - mo
    all_rows, all_cols = slabs * rows, modes * cols
    kx_count = 2 * slabs

    loads = [
        pltpu.make_async_copy(x_hbm, xv, lsem.at[0]),
        pltpu.make_async_copy(cot_hbm, cv, lsem.at[1]),
        pltpu.make_async_copy(w_hbm, wv, lsem.at[2]),
    ]
    for load in loads:
        load.start()

    barrier = pltpu.get_barrier_semaphore()

    def greet(k, carry):
        pl.semaphore_signal(barrier, inc=1, device_id={"slab": lax.rem(me + k, slabs)}, device_id_type=MESH)
        return carry

    lax.fori_loop(1, slabs, greet, 0)
    for k in range(1, chans):
        pl.semaphore_signal(barrier, inc=1, device_id={"chan": lax.rem(ch + k, chans)}, device_id_type=MESH)
    pl.semaphore_signal(barrier, inc=1, device_id={"mode": other}, device_id_type=MESH)

    def to_mode(slot, src, dst):
        return pltpu.make_async_remote_copy(
            src_ref=src, dst_ref=dst, send_sem=msend.at[slot], recv_sem=mrecv.at[slot],
            device_id={"mode": other}, device_id_type=MESH,
        )

    def to_slabs(slot, src_of, dst):
        def one(n, carry):
            far = slabs // 2
            k = jnp.where(n % 2 == 0, far - n // 2, far + (n + 1) // 2)
            pltpu.make_async_remote_copy(
                src_ref=src_of(k), dst_ref=dst.at[slabs - k], send_sem=ssend.at[slot], recv_sem=srecv.at[slot],
                device_id={"slab": lax.rem(me + k, slabs)}, device_id_type=MESH,
            ).start()
            return carry

        lax.fori_loop(0, slabs - 1, one, 0)

    def wait_bytes(ref, sem):
        pltpu.make_async_copy(ref, ref, sem).wait()

    lane = iota((8, LANES), 1)
    real_part = lane % 32 < 16

    def turned(v):
        re = iota(v.shape, 1) % 32 < 16
        return jnp.where(re, pltpu.roll(v, LANES - 16, 1), -pltpu.roll(v, 16, 1))

    def column_angles(n, w):
        holder = jnp.where(n < LANES, mo, other)
        freq = holder * 16 + n % 16
        cell = mo * cols + w
        return freq * cell + jnp.where(n % 32 < 16, all_cols // 4, all_cols // 2)

    shape = (cols, 2 * LANES)
    tch[...], tcl[...] = split(sine(column_angles(iota(shape, 1), iota(shape, 0)), all_cols))

    def row_angles(k, n, mirror):
        kx = 2 * lax.rem(me + k // 8, slabs) + (k % 8) // 4
        kx = jnp.where(kx < kx_count // 2, kx, kx + all_rows - kx_count)
        half = LANES
        cell = me * rows + n % rows
        angle = kx * cell + jnp.where(n < half, all_rows // 4, 0)
        same = (k % 4) == ((n % half) // rows)
        return jnp.where(same, sine(angle, all_rows), 0.0)

    shape = (8 * slabs, 2 * LANES)
    fh[...], fl[...] = split(row_angles(iota(shape, 0), iota(shape, 1), False))

    def column_forward(a, values):
        d = dot3(split(values), (tch[...], tcl[...]))
        block = (iota((rows, 2 * LANES), 1) % LANES) // 32
        packed = d[:rows]
        for b in range(1, 4):
            packed = jnp.where(block == b, d[b * rows : (b + 1) * rows], packed)
        own_cols[pl.ds(a * rows, rows), :] = packed[:, :LANES]
        return packed[:, LANES:]

    loads[0].wait()

    def first_chunk(a, carry):
        values = xv[pl.ds(a * chunk, chunk), :]
        tx_cols[0, pl.ds(a * rows, rows), :] = column_forward(a, values)
        return carry

    lax.fori_loop(0, 4, first_chunk, 0)
    pl.semaphore_wait(barrier, slabs - 1 + chans - 1 + 1)

    def rows_forward(turn):
        copy = to_mode(turn, tx_cols.at[turn], rx_cols.at[turn])
        copy.start()
        copy.wait()
        lined = own_cols[...] + rx_cols[turn]
        both = jnp.concatenate([lined, turned(lined)], axis=0)
        partial = dot3((fh[...], fl[...]), split(both))
        tx_rows[turn] = partial.reshape(slabs, 8, LANES)
        to_slabs(turn, lambda k: tx_rows.at[turn, k], rx_rows.at[turn])

    def owned(turn):
        wait_bytes(rx_rows.at[turn, pl.ds(1, slabs - 1)], srecv.at[turn])
        total = tx_rows[turn, 0]
        for j in range(1, slabs):
            total = total + rx_rows[turn, j]
        return total

    rows_forward(0)

    shape = (2 * LANES, cols)
    tth[...], ttl[...] = split(sine(column_angles(iota(shape, 0), iota(shape, 1)), all_cols))
    shape = (2 * LANES, 8 * slabs)
    fth[...], ftl[...] = split(row_angles(iota(shape, 1), iota(shape, 0), True))

    sub = iota((8, LANES), 0)
    keep_col = jnp.zeros((8, LANES), jnp.int32)
    keep_row = jnp.zeros((8, LANES), jnp.int32)
    for c in range(16):
        here = (sub % 4 == c // 4) & (lane // 32 == c % 4)
        keep_col = jnp.where(here, limit[0, ch * 16 + c], keep_col)
        keep_row = jnp.where(here, limit[1, ch * 16 + c], keep_row)
    col_freq = mo * 16 + lane % 16
    row_freq = me * 2 + sub // 4
    kept = (col_freq < keep_col) & ((row_freq < keep_row) | (kx_count - row_freq < keep_row))
    scale = jnp.where(col_freq == 0, 1.0, 2.0) / (all_rows * all_cols)
    weights = jnp.where(kept, scale, 0.0)

    sub16 = iota((16, LANES), 0)
    lane16 = iota((16, LANES), 1)
    reads = jnp.zeros((16, LANES), jnp.int32)
    for o in range(16 * chans):
        reads = jnp.where((sub16 == o // 4) & (lane16 // 32 == o % 4), width[o], reads)

    loads[2].wait()

    def weights_in(pair, carry):
        parts = []
        for t in range(4):
            for p in range(2):
                parts.append(wv[2 * pair + t // 2, pl.ds(2 * p + t % 2, 16, stride=4), :])
        zs[...] = jnp.concatenate(parts, axis=0).T
        by_low = [zs[pl.ds(b, 16, stride=4), :] for b in range(4)]
        for t in range(4):
            i = 2 * pair + t // 2
            tile = jnp.zeros((16, LANES), jnp.float32)
            for b in range(4):
                shift = 32 * ((b - t) % 4)
                moved = pltpu.roll(by_low[b], shift, 1) if shift else by_low[b]
                tile = jnp.where(lane16 // 32 == b, moved, tile)
            tile = jnp.where(ch * 16 + i < reads, tile, 0.0)
            for d in range(chans):
                wt[i, d, pl.ds(4 * (t % 2), 4), :] = tile[4 * d : 4 * d + 4]
        return carry

    lax.fori_loop(0, 8, weights_in, 0)

    spectra = owned(0)
    for a in range(4):
        e = jnp.where(
            sub < 4,
            jnp.broadcast_to(spectra[a : a + 1], (8, LANES)),
            jnp.broadcast_to(spectra[4 + a : 5 + a], (8, LANES)),
        )
        rolled = [e] + [pltpu.roll(e, 16 * m, 1) for m in range(1, 8)]
        for q in range(8):
            copies = rolled[(0 - q) % 8]
            for t in range(1, 8):
                copies = jnp.where(lane // 16 == t, rolled[(t - q) % 8], copies)
            sv[4 * a + q // 2, q % 2] = copies

    zero = jnp.zeros((8, LANES), jnp.float32)

    def contract(i, sums):
        s_re, s_im = sv[i, 0], sv[i, 1]
        first = tuple(sums[d] + s_re * wt[i, d] for d in range(chans))
        second = tuple(sums[chans + d] + s_im * wt[i, d] for d in range(chans))
        return first + second

    sums = lax.fori_loop(0, 16, contract, (zero,) * (2 * chans), unroll=4)
    for d in range(chans):
        tx_chan[d] = sums[d] - turned(sums[chans + d])

    def to_chan(slot, k, src, dst):
        return pltpu.make_async_remote_copy(
            src_ref=src, dst_ref=dst, send_sem=csend.at[slot], recv_sem=crecv.at[slot],
            device_id={"chan": lax.rem(ch + k, chans)}, device_id_type=MESH,
        )

    for k in range(1, chans):
        to_chan(0, k, tx_chan.at[lax.rem(ch + k, chans)], rx_chan.at[chans - 1 - k]).start()
    wait_bytes(rx_chan, crecv.at[0])
    modes_out = tx_chan[ch]
    for k in range(chans - 1):
        modes_out = modes_out + rx_chan[k]

    def everywhere(turn, tile):
        tile_tx[turn] = tile
        rx_modes[turn, 0] = tile
        to_slabs(2 + turn, lambda k: tile_tx.at[turn], rx_modes.at[turn])

    def rows_back(turn):
        wait_bytes(rx_modes.at[turn, pl.ds(1, slabs - 1)], srecv.at[2 + turn])
        found = rx_modes[turn].reshape(8 * slabs, LANES)
        both = dot3((fth[...], ftl[...]), split(found))
        own_g[turn] = both[:LANES] - turned(both[LANES:])
        copy = to_mode(2 + turn, own_g.at[turn], rx_g.at[turn])
        copy.start()
        copy.wait()

    def column_back(turn, a):
        g = jnp.concatenate(
            [own_g[turn, pl.ds(a * rows, rows), :], rx_g[turn, pl.ds(a * rows, rows), :]], axis=1
        )
        block = (iota(g.shape, 1) % LANES) // 32
        spread = jnp.concatenate([jnp.where(block == b, g, 0.0) for b in range(4)], axis=0)
        return dot3(split(spread), (tth[...], ttl[...]))

    everywhere(0, modes_out * weights)
    loads[1].wait()
    rows_back(0)

    def gelu_chunk(a, carry):
        gates, biases = carry
        branch = column_back(0, a)
        grads = []
        for b in range(4):
            c = 4 * a + b
            here = pl.ds(c * rows, rows)
            x = xv[here, :]
            v = branch[b * rows : (b + 1) * rows] + gain[c] * x + bias[c]
            v2 = v * v
            t = jnp.tanh(GELU_SLOPE * (v + GELU_CUBE * (v2 * v)))
            cdf = 0.5 * (1.0 + t)
            ov[here, :] = v * cdf
            slope = cdf + (0.5 * GELU_SLOPE) * (v * (1.0 - t * t)) * (1.0 + (3.0 * GELU_CUBE) * v2)
            grad = cv[here, :] * slope
            gv[here, :] = grad
            grads.append(grad)
            gate = jnp.sum(jnp.sum(grad * x, axis=0, keepdims=True), axis=1, keepdims=True)
            plain = jnp.sum(jnp.sum(grad, axis=0, keepdims=True), axis=1, keepdims=True)
            spot = iota((1, LANES), 1) == c
            gates = jnp.where(spot, gate, gates)
            biases = jnp.where(spot, plain, biases)
        tx_cols[1, pl.ds(a * rows, rows), :] = column_forward(a, jnp.concatenate(grads, axis=0))
        here = pl.ds(a * chunk, chunk)
        pltpu.make_async_copy(ov.at[here, :], out_hbm.at[here, :], osem.at[0]).start()
        return gates, biases

    empty = jnp.zeros((1, LANES), jnp.float32)
    gates, biases = lax.fori_loop(0, 4, gelu_chunk, (empty, empty))
    rows_forward(1)

    red_pair[0] = jnp.concatenate([gates, biases], axis=0)
    copy = to_mode(4, red_pair.at[0], red_pair.at[1])
    copy.start()
    copy.wait()
    red_pair[2] = red_pair[0] + red_pair[1]
    to_slabs(4, lambda k: red_pair.at[2], red_all)

    g_chan[ch] = owned(1) * weights
    for k in range(1, chans):
        to_chan(1, k, g_chan.at[ch], g_chan.at[ch]).start()
    wait_bytes(g_chan.at[pl.ds(0, chans - 1)], crecv.at[1])
    g_all = [g_chan[d] for d in range(chans)]
    g_turned = [turned(g) for g in g_all]

    def contract_back(i):
        first, second = zero, zero
        for d in range(chans):
            w = wt[i, d]
            first = first + w * g_all[d]
            second = second + w * g_turned[d]
        v = jnp.where(real_part, first + pltpu.roll(first, 16, 1), second + pltpu.roll(second, 16, 1))
        v = v + pltpu.roll(v, 32, 1)
        return v + pltpu.roll(v, 64, 1)

    back = zero
    for a in range(4):
        m = contract_back(4 * a)
        for b in range(1, 4):
            m = jnp.where(lane // 32 == b, contract_back(4 * a + b), m)
        for x in range(2):
            row = jnp.sum(m[4 * x : 4 * x + 4], axis=0, keepdims=True)
            back = jnp.where(sub == 4 * x + a, jnp.broadcast_to(row, (8, LANES)), back)
    everywhere(1, back)

    def weights_out(pair, carry):
        tiles = []
        for t in range(4):
            i = 2 * pair + t // 2
            if t % 2 == 0:
                s_re, s_im = sv[i, 0], sv[i, 1]
                made = [s_re * g_all[d] + s_im * g_turned[d] for d in range(chans)]
            parts = [made[d][4 * (t % 2) : 4 * (t % 2) + 4] for d in range(chans)]
            tile = jnp.concatenate(parts, axis=0)
            tiles.append(jnp.where(ch * 16 + i < reads, tile, 0.0))
        for b in range(4):
            low = jnp.zeros((16, LANES), jnp.float32)
            for t in range(4):
                shift = 32 * ((t - b) % 4)
                moved = pltpu.roll(tiles[t], shift, 1) if shift else tiles[t]
                low = jnp.where(lane16 // 32 == t, moved, low)
            zs[pl.ds(b, 16, stride=4), :] = low
        back_rows = zs[...].T
        for t in range(4):
            for p in range(2):
                at = 32 * t + 16 * p
                sgv[2 * pair + t // 2, pl.ds(2 * p + t % 2, 16, stride=4), :] = back_rows[at : at + 16]
        return carry

    lax.fori_loop(0, 8, weights_out, 0)
    sgrad_copy = pltpu.make_async_copy(sgv, sgrad_hbm, osem.at[1])
    sgrad_copy.start()

    wait_bytes(red_all.at[pl.ds(1, slabs - 1)], srecv.at[4])
    total = red_pair[2]
    for j in range(1, slabs):
        total = total + red_all[j]
    gate_ref[...] = total[0:1, :16]
    bgrad_ref[...] = total[1:2, :16]

    wait_bytes(ov, osem.at[0])
    rows_back(1)

    def last_chunk(a, carry):
        branch = column_back(1, a)
        for b in range(4):
            c = 4 * a + b
            here = pl.ds(c * rows, rows)
            ov[here, :] = branch[b * rows : (b + 1) * rows] + gain[c] * gv[here, :]
        here = pl.ds(a * chunk, chunk)
        pltpu.make_async_copy(ov.at[here, :], fgrad_hbm.at[here, :], osem.at[2]).start()
        return carry

    lax.fori_loop(0, 4, last_chunk, 0)
    sgrad_copy.wait()
    for turn in range(2):
        wait_bytes(tx_rows.at[turn, pl.ds(1, slabs - 1)], ssend.at[turn])
        wait_bytes(rx_modes.at[turn, pl.ds(1, slabs - 1)], ssend.at[2 + turn])
        wait_bytes(rx_chan, csend.at[turn])
    wait_bytes(red_all.at[pl.ds(1, slabs - 1)], ssend.at[4])
    wait_bytes(ov, osem.at[2])


def local(source_field, cotangent, spectral_weight, skip_gain, channel_bias, mode_limit, width_limit):
    channels, rows, cols = source_field.shape
    slabs, chans, modes = lax.axis_size("slab"), lax.axis_size("chan"), lax.axis_size("mode")
    outs = spectral_weight.shape[1]
    assert (channels, rows, modes, outs) == (16, 32, 2, 16 * chans)
    assert spectral_weight.shape[2:] == (16, 2, 2)
    flat = (channels * rows, cols)
    w = spectral_weight.transpose(0, 2, 3, 4, 1).reshape(channels, 64, outs)
    f32, bf16 = jnp.float32, jnp.bfloat16
    vmem = pltpu.VMEM
    any_space = pl.BlockSpec(memory_space=pl.ANY)
    smem = pl.BlockSpec(memory_space=pltpu.SMEM)
    row = pl.BlockSpec(memory_space=pltpu.VMEM)
    square = (LANES, LANES)
    out, fgrad, sgrad, gate, bgrad = pl.pallas_call(
        functools.partial(kernel, (slabs, chans, modes, rows, cols)),
        out_shape=(
            jax.ShapeDtypeStruct(flat, f32),
            jax.ShapeDtypeStruct(flat, f32),
            jax.ShapeDtypeStruct(w.shape, f32),
            jax.ShapeDtypeStruct((1, channels), f32),
            jax.ShapeDtypeStruct((1, channels), f32),
        ),
        in_specs=[any_space] * 3 + [smem] * 4,
        out_specs=[any_space] * 3 + [row] * 2,
        scratch_shapes=[
            vmem(flat, f32), vmem(flat, f32), vmem(w.shape, f32), vmem(flat, f32), vmem(flat, f32),
            vmem((cols, 2 * LANES), bf16), vmem((cols, 2 * LANES), bf16),
            vmem((2 * LANES, cols), bf16), vmem((2 * LANES, cols), bf16),
            vmem((8 * slabs, 2 * LANES), bf16), vmem((8 * slabs, 2 * LANES), bf16),
            vmem((2 * LANES, 8 * slabs), bf16), vmem((2 * LANES, 8 * slabs), bf16),
            vmem((channels, chans, 8, LANES), f32), vmem((outs, LANES), f32),
            vmem((channels, 2, 8, LANES), f32), vmem(w.shape, f32),
            vmem(square, f32), vmem((2, *square), f32), vmem((2, *square), f32),
            vmem((2, slabs, 8, LANES), f32), vmem((2, slabs, 8, LANES), f32),
            vmem((chans, 8, LANES), f32), vmem((chans - 1, 8, LANES), f32),
            vmem((2, 8, LANES), f32), vmem((2, slabs, 8, LANES), f32),
            vmem((2, *square), f32), vmem((2, *square), f32),
            vmem((chans, 8, LANES), f32), vmem((3, 2, LANES), f32), vmem((slabs, 2, LANES), f32),
            pltpu.SemaphoreType.DMA((3,)), pltpu.SemaphoreType.DMA((3,)),
            pltpu.SemaphoreType.DMA((5,)), pltpu.SemaphoreType.DMA((5,)),
            pltpu.SemaphoreType.DMA((5,)), pltpu.SemaphoreType.DMA((5,)),
            pltpu.SemaphoreType.DMA((2,)), pltpu.SemaphoreType.DMA((2,)),
        ],
        compiler_params=pltpu.CompilerParams(collective_id=0, has_side_effects=True, vmem_limit_bytes=40 << 20),
        name="fno_layer",
    )(
        source_field.reshape(flat), cotangent.reshape(flat), w, skip_gain, channel_bias,
        mode_limit.T, width_limit,
    )
    sgrad = sgrad.reshape(channels, 16, 2, 2, outs).transpose(0, 4, 1, 2, 3)
    return (
        out.reshape(source_field.shape), fgrad.reshape(source_field.shape), sgrad,
        gate.reshape(channels), bgrad.reshape(channels),
    )


def solution(mesh):
    field = P(("member", "chan"), "slab", "mode")
    weight = P(("member", "chan"), None, "mode", None, "slab")
    channel = P(("member", "chan"))
    return jax.shard_map(
        local,
        mesh=mesh,
        in_specs=(field, field, weight, channel, channel, P("member", None), P("member")),
        out_specs=(field, field, weight, channel, channel),
        check_vma=False,
    )
```

```python
import functools
import math

import jax
import jax.numpy as jnp
from jax import lax
from jax.experimental import pallas as pl
from jax.experimental.pallas import tpu as pltpu
from jax.sharding import PartitionSpec as P

MESH = pl.DeviceIdType.MESH
LANES = 128
GELU_SLOPE = math.sqrt(2.0 / math.pi)
GELU_CUBE = 0.044715


def slab_offsets(slabs):
    hubs = slabs // 8 - 1
    far = [4 * m for m in range(1, hubs + 1)]
    found = [0, slabs // 2] + far + [-k for k in far]
    for sign in (1, -1):
        for j in range(1, 4):
            found += [sign * (j + 4 * m) for m in range(hubs + 1)]
    return found


def offset_of(slot, slabs):
    hubs = slabs // 8 - 1
    first = 2 + 2 * hubs
    near = jnp.where(slot < 2 + hubs, 4 * (slot - 1), -4 * (slot - 1 - hubs))
    group, m = (slot - first) // (hubs + 1), (slot - first) % (hubs + 1)
    behind = jnp.where(group < 3, 1 + group + 4 * m, -(group - 2) - 4 * m)
    found = jnp.where(slot < first, near, behind)
    return jnp.where(slot == 0, 0, jnp.where(slot == 1, slabs // 2, found))


def split(x):
    high = x.astype(jnp.bfloat16)
    low = (x - high.astype(jnp.float32)).astype(jnp.bfloat16)
    return high, low


def dot3(a, b):
    (ah, al), (bh, bl) = a, b
    dot = functools.partial(jnp.dot, preferred_element_type=jnp.float32)
    return dot(ah, bh) + (dot(ah, bl) + dot(al, bh))


def sine(turns, extent):
    half, quarter = extent // 2, extent // 4
    t = ((turns + half) & (extent - 1)) - half
    t = jnp.where(t > quarter, half - t, jnp.where(t < -quarter, -half - t, t))
    v = t.astype(jnp.float32) * (2.0 * math.pi / extent)
    s = v * v
    poly = -2.5052108e-8
    for c in (2.7557319e-6, -1.9841270e-4, 8.3333333e-3, -1.6666667e-1, 1.0):
        poly = poly * s + c
    return poly * v


def iota(shape, dim):
    return lax.broadcasted_iota(jnp.int32, shape, dim)


def kernel(
    dims,
    x_hbm, cot_hbm, w_hbm, gain_hbm, bias_hbm, limit_hbm, width_hbm,
    ov, gv, sgv, gate_ref, bgrad_ref, last_own, last_rx, tth, ttl,
    xv, cv, wv, gain, bias, limit, width, tch, tcl, fh, fl, fth, ftl,
    wt, zs, sv,
    own_cols, tx_cols, rx_cols, tx_rows, rx_near, rx_anti, tx_far, rx_far, tx_chan, rx_chan, rx_modes,
    own_g, rx_g, g_chan, red_pair, red_near, red_far,
    lsem, msend, mrecv, ssend, nrecv, frecv, hrecv, arecv, csend, crecv, rsend, rrecv,
):
    slabs, chans, modes, rows, cols = dims
    chunk = 4 * rows
    me, ch, mo = lax.axis_index("slab"), lax.axis_index("chan"), lax.axis_index("mode")
    other = 1 - mo
    all_rows, all_cols = slabs * rows, modes * cols
    kx_count = 2 * slabs

    scope = jax.named_scope
    barrier = pltpu.get_barrier_semaphore()

    hubs = slabs // 8 - 1
    offsets = slab_offsets(slabs)
    partners = [k for k in offsets if k and (k % 4 == 0 or abs(k) < 4) and k != slabs // 2]

    def slab_at(k):
        return {"slab": (me + k + slabs) & (slabs - 1)}

    with scope("greet"):
        for k in partners:
            pl.semaphore_signal(barrier, inc=1, device_id=slab_at(k), device_id_type=MESH)
    for k in range(1, chans):
        pl.semaphore_signal(barrier, inc=1, device_id={"chan": lax.rem(ch + k, chans)}, device_id_type=MESH)
    pl.semaphore_signal(barrier, inc=1, device_id={"mode": other}, device_id_type=MESH)

    pairs = (
        (x_hbm, xv), (cot_hbm, cv), (w_hbm, wv), (limit_hbm, limit), (width_hbm, width),
        (gain_hbm, gain), (bias_hbm, bias),
    )
    loads = [pltpu.make_async_copy(a, b, lsem.at[n]) for n, (a, b) in enumerate(pairs)]
    for load in loads:
        load.start()
    def to_mode(slot, src, dst):
        return pltpu.make_async_remote_copy(
            src_ref=src, dst_ref=dst, send_sem=msend.at[slot], recv_sem=mrecv.at[slot],
            device_id={"mode": other}, device_id_type=MESH,
        )

    def to_slab(k, src, dst, send_sem, recv_sem):
        pltpu.make_async_remote_copy(
            src_ref=src, dst_ref=dst, send_sem=send_sem, recv_sem=recv_sem,
            device_id=slab_at(k), device_id_type=MESH,
        ).start()

    def wait_bytes(ref, sem):
        pltpu.make_async_copy(ref, ref, sem).wait()

    lane = iota((8, LANES), 1)
    real_part = lane % 32 < 16

    def turned(v):
        re = iota(v.shape, 1) & 31 < 16
        return jnp.where(re, pltpu.roll(v, LANES - 16, 1), -pltpu.roll(v, 16, 1))

    def column_angles(n, w):
        holder = jnp.where(n < LANES, mo, other)
        freq = holder * 16 + (n & 15)
        cell = mo * cols + w
        return freq * cell + jnp.where(n & 31 < 16, all_cols // 4, all_cols // 2)

    with scope("column_table"):
        shape = (cols, 2 * LANES)
        tch[...], tcl[...] = split(sine(column_angles(iota(shape, 1), iota(shape, 0)), all_cols))

    def row_angles(k, n):
        kx = 2 * ((me + offset_of(k >> 3, slabs) + slabs) & (slabs - 1)) + ((k >> 2) & 1)
        kx = jnp.where(kx < kx_count // 2, kx, kx + all_rows - kx_count)
        half = LANES
        cell = me * rows + (n & (rows - 1))
        angle = kx * cell + jnp.where(n < half, all_rows // 4, 0)
        same = (k & 3) == ((n & (half - 1)) // rows)
        return jnp.where(same, sine(angle, all_rows), 0.0)

    def column_forward(a, values):
        d = dot3(split(values), (tch[...], tcl[...]))
        block = (iota((rows, 2 * LANES), 1) % LANES) // 32
        packed = d[:rows]
        for b in range(1, 4):
            packed = jnp.where(block == b, d[b * rows : (b + 1) * rows], packed)
        own_cols[pl.ds(a * rows, rows), :] = packed[:, :LANES]
        return packed[:, LANES:]

    with scope("load_wait"):
        loads[0].wait()

    def first_chunk(a, carry):
        values = xv[pl.ds(a * chunk, chunk), :]
        tx_cols[0, pl.ds(a * rows, rows), :] = column_forward(a, values)
        return carry

    with scope("first_columns"):
        lax.fori_loop(0, 4, first_chunk, 0)
    with scope("barrier_wait"):
        pl.semaphore_wait(barrier, len(partners) + chans - 1 + 1)

    def rows_forward(turn):
        copy = to_mode(turn, tx_cols.at[turn], rx_cols.at[turn])
        copy.start()
        if turn == 0:
            with scope("row_table"):
                shape = (8 * slabs, 2 * LANES)
                fh[...], fl[...] = split(row_angles(iota(shape, 0), iota(shape, 1)))
        with scope("columns_pair"):
            copy.wait()
        with scope("rows_dot"):
            lined = own_cols[...] + rx_cols[turn]
            both = jnp.concatenate([lined, turned(lined)], axis=0)
            partial = dot3((fh[...], fl[...]), split(both))
            tx_rows[turn] = partial.reshape(slabs, 8, LANES)
        with scope("rows_send"):
            for m in range(hubs, -1, -1):
                if m == hubs:
                    to_slab(4, tx_rows.at[turn, 1], rx_anti.at[turn], ssend.at[turn, 0], nrecv.at[turn, 2, 0])
                for j in (3, 2, 1):
                    for side in range(2):
                        slot = 2 + 2 * hubs + (3 * side + j - 1) * (hubs + 1) + m
                        to_slab(
                            j if side == 0 else -j, tx_rows.at[turn, slot], rx_near.at[turn, side, m, j - 1],
                            ssend.at[turn, 1], nrecv.at[turn, side, m],
                        )

    def owned(turn):
        for m in range(hubs, 0, -1):
            for side in range(2):
                with scope("near_wait"):
                    wait_bytes(rx_near.at[turn, side, m], nrecv.at[turn, side, m])
                slot = 1 + hubs * side + m
                total = tx_rows[turn, slot]
                for j in range(3):
                    total = total + rx_near[turn, side, m, j]
                if m == hubs and side == 0:
                    wait_bytes(rx_anti.at[turn], nrecv.at[turn, 2, 0])
                    total = total + rx_anti[turn]
                tx_far[turn, slot - 2] = total
                to_slab(
                    4 * m if side == 0 else -4 * m, tx_far.at[turn, slot - 2], rx_far.at[turn, slot - 2],
                    ssend.at[turn, 2], frecv.at[turn],
                )
        total = tx_rows[turn, 0]
        for side in range(2):
            wait_bytes(rx_near.at[turn, side, 0], nrecv.at[turn, side, 0])
            for j in range(3):
                total = total + rx_near[turn, side, 0, j]
        with scope("rows_wait"):
            wait_bytes(rx_far.at[turn], frecv.at[turn])
        for n in range(2 * hubs):
            total = total + rx_far[turn, n]
        return total

    rows_forward(0)

    with scope("back_tables"):
        shape = (2 * LANES, cols)
        tth[...], ttl[...] = split(sine(column_angles(iota(shape, 0), iota(shape, 1)), all_cols))
        shape = (2 * LANES, 8 * slabs)
        fth[...], ftl[...] = split(row_angles(iota(shape, 1), iota(shape, 0)))

    for load in loads[3:]:
        load.wait()
    sub = iota((8, LANES), 0)
    keep_col = jnp.zeros((8, LANES), jnp.int32)
    keep_row = jnp.zeros((8, LANES), jnp.int32)
    for c in range(16):
        here = (sub % 4 == c // 4) & (lane // 32 == c % 4)
        keep_col = jnp.where(here, limit[0, ch * 16 + c], keep_col)
        keep_row = jnp.where(here, limit[1, ch * 16 + c], keep_row)
    col_freq = mo * 16 + lane % 16
    row_freq = me * 2 + sub // 4
    kept = (col_freq < keep_col) & ((row_freq < keep_row) | (kx_count - row_freq < keep_row))
    scale = jnp.where(col_freq == 0, 1.0, 2.0) / (all_rows * all_cols)
    weights = jnp.where(kept, scale, 0.0)

    sub16 = iota((16, LANES), 0)
    lane16 = iota((16, LANES), 1)
    reads = jnp.zeros((16, LANES), jnp.int32)
    for o in range(16 * chans):
        reads = jnp.where((sub16 == o // 4) & (lane16 // 32 == o % 4), width[o], reads)

    loads[2].wait()

    def weights_in(pair, carry):
        parts = []
        for t in range(4):
            for p in range(2):
                parts.append(wv[2 * pair + t // 2, pl.ds(2 * p + t % 2, 16, stride=4), :])
        zs[...] = jnp.concatenate(parts, axis=0).T
        by_low = [zs[pl.ds(b, 16, stride=4), :] for b in range(4)]
        for t in range(4):
            i = 2 * pair + t // 2
            tile = jnp.zeros((16, LANES), jnp.float32)
            for b in range(4):
                shift = 32 * ((b - t) % 4)
                moved = pltpu.roll(by_low[b], shift, 1) if shift else by_low[b]
                tile = jnp.where(lane16 // 32 == b, moved, tile)
            tile = jnp.where(ch * 16 + i < reads, tile, 0.0)
            for d in range(chans):
                wt[i, d, pl.ds(4 * (t % 2), 4), :] = tile[4 * d : 4 * d + 4]
        return carry

    with jax.named_scope("weights_in"):
        lax.fori_loop(0, 8, weights_in, 0)

    spectra = owned(0)
    for a in range(4):
        e = jnp.where(
            sub < 4,
            jnp.broadcast_to(spectra[a : a + 1], (8, LANES)),
            jnp.broadcast_to(spectra[4 + a : 5 + a], (8, LANES)),
        )
        rolled = [e] + [pltpu.roll(e, 16 * m, 1) for m in range(1, 8)]
        for q in range(8):
            copies = rolled[(0 - q) % 8]
            for t in range(1, 8):
                copies = jnp.where(lane // 16 == t, rolled[(t - q) % 8], copies)
            sv[4 * a + q // 2, q % 2] = copies

    zero = jnp.zeros((8, LANES), jnp.float32)

    def contract(i, sums):
        s_re, s_im = sv[i, 0], sv[i, 1]
        first = tuple(sums[d] + s_re * wt[i, d] for d in range(chans))
        second = tuple(sums[chans + d] + s_im * wt[i, d] for d in range(chans))
        return first + second

    sums = lax.fori_loop(0, 16, contract, (zero,) * (2 * chans), unroll=4)
    for d in range(chans):
        tx_chan[d] = sums[d] - turned(sums[chans + d])

    def to_chan(slot, k, src, dst):
        return pltpu.make_async_remote_copy(
            src_ref=src, dst_ref=dst, send_sem=csend.at[slot], recv_sem=crecv.at[slot],
            device_id={"chan": lax.rem(ch + k, chans)}, device_id_type=MESH,
        )

    for k in range(1, chans):
        to_chan(0, k, tx_chan.at[lax.rem(ch + k, chans)], rx_chan.at[chans - 1 - k]).start()
    with scope("chan_wait"):
        wait_bytes(rx_chan, crecv.at[0])
    modes_out = tx_chan[ch]
    for k in range(chans - 1):
        modes_out = modes_out + rx_chan[k]

    def everywhere(turn, tile):
        rx = rx_modes.at[turn]
        rx[0] = tile
        with scope("modes_send"):
            for m in range(hubs, 0, -1):
                for side, k in enumerate((4 * m, -4 * m)):
                    to_slab(
                        k, rx.at[0], rx.at[offsets.index(-k)], ssend.at[2 + turn, 0], hrecv.at[turn, m - 1, side]
                    )
            for j in (3, 2, 1):
                for k in (j, -j):
                    to_slab(k, rx.at[0], rx.at[offsets.index(-k)], ssend.at[2 + turn, 0], arecv.at[turn])

    def passed_on(turn):
        rx = rx_modes.at[turn]
        for m in range(1, hubs + 1):
            for side in range(2):
                sign = 1 if side == 0 else -1
                held = rx.at[offsets.index(-sign * 4 * m)]
                with scope("hub_wait"):
                    wait_bytes(held, hrecv.at[turn, m - 1, side])
                for j in (4, 3, 2, 1) if m == hubs and side == 0 else (3, 2, 1):
                    there = rx.at[1 if j == 4 else offsets.index(-sign * (4 * m + j))]
                    to_slab(sign * j, held, there, ssend.at[2 + turn, 1], arecv.at[turn])

    def rows_back(turn):
        with scope("modes_wait"):
            wait_bytes(rx_modes.at[turn, pl.ds(0, slabs - 1 - 2 * hubs)], arecv.at[turn])
        with scope("back_dot"):
            found = rx_modes[turn].reshape(8 * slabs, LANES)
            both = dot3((fth[...], ftl[...]), split(found))
            own_g[turn] = both[:LANES] - turned(both[LANES:])
        with scope("back_pair"):
            copy = to_mode(2 + turn, own_g.at[turn], rx_g.at[turn])
            copy.start()
            copy.wait()

    everywhere(0, modes_out * weights)
    loads[1].wait()
    passed_on(0)
    rows_back(0)

    def gelu_chunk(a, carry):
        gates, biases = carry
        branch = column_synthesis(own_g.at[0], rx_g.at[0], a, rows, (tth, ttl))
        grads = []
        for b in range(4):
            c = 4 * a + b
            here = pl.ds(c * rows, rows)
            x = xv[here, :]
            v = branch[b * rows : (b + 1) * rows] + gain[c] * x + bias[c]
            v2 = v * v
            t = jnp.tanh(GELU_SLOPE * (v + GELU_CUBE * (v2 * v)))
            cdf = 0.5 * (1.0 + t)
            ov[here, :] = v * cdf
            slope = cdf + (0.5 * GELU_SLOPE) * (v * (1.0 - t * t)) * (1.0 + (3.0 * GELU_CUBE) * v2)
            grad = cv[here, :] * slope
            gv[here, :] = gain[c] * grad
            grads.append(grad)
            gate = jnp.sum(jnp.sum(grad * x, axis=0, keepdims=True), axis=1, keepdims=True)
            plain = jnp.sum(jnp.sum(grad, axis=0, keepdims=True), axis=1, keepdims=True)
            spot = iota((1, LANES), 1) == c
            gates = jnp.where(spot, gate, gates)
            biases = jnp.where(spot, plain, biases)
        tx_cols[1, pl.ds(a * rows, rows), :] = column_forward(a, jnp.concatenate(grads, axis=0))
        return gates, biases

    empty = jnp.zeros((1, LANES), jnp.float32)
    with scope("gelu"):
        gates, biases = lax.fori_loop(0, 4, gelu_chunk, (empty, empty))
    rows_forward(1)

    red_pair[0] = jnp.concatenate([gates, biases], axis=0)
    with scope("pair_sums"):
        copy = to_mode(4, red_pair.at[0], red_pair.at[1])
        copy.start()
        copy.wait()
        red_pair[2] = red_pair[0] + red_pair[1]
        for j in range(1, 4):
            pltpu.make_async_remote_copy(
                src_ref=red_pair.at[2], dst_ref=red_near.at[j - 1], send_sem=rsend.at[0], recv_sem=rrecv.at[0],
                device_id={"slab": me ^ j}, device_id_type=MESH,
            ).start()

    g_chan[ch] = owned(1) * weights
    for k in range(1, chans):
        to_chan(1, k, g_chan.at[ch], g_chan.at[ch]).start()
    with scope("chan_wait_two"):
        wait_bytes(g_chan.at[pl.ds(0, chans - 1)], crecv.at[1])
    g_all = [g_chan[d] for d in range(chans)]
    g_turned = [turned(g) for g in g_all]

    def contract_back(i):
        first, second = zero, zero
        for d in range(chans):
            w = wt[i, d]
            first = first + w * g_all[d]
            second = second + w * g_turned[d]
        v = jnp.where(real_part, first + pltpu.roll(first, 16, 1), second + pltpu.roll(second, 16, 1))
        v = v + pltpu.roll(v, 32, 1)
        return v + pltpu.roll(v, 64, 1)

    back = zero
    for a in range(4):
        m = contract_back(4 * a)
        for b in range(1, 4):
            m = jnp.where(lane // 32 == b, contract_back(4 * a + b), m)
        for x in range(2):
            row = jnp.sum(m[4 * x : 4 * x + 4], axis=0, keepdims=True)
            back = jnp.where(sub == 4 * x + a, jnp.broadcast_to(row, (8, LANES)), back)
    everywhere(1, back)

    with scope("sums_near"):
        wait_bytes(red_near, rrecv.at[0])
        total = red_pair[2]
        for j in range(3):
            total = total + red_near[j]
        red_pair[3] = total
        for m in range(1, hubs + 1):
            for side, k in enumerate((4 * m, -4 * m)):
                last = side * m == hubs
                to_slab(k, red_pair.at[3], red_far.at[hubs * side + m - 1], rsend.at[1], rrecv.at[2 if last else 1])

    def weights_out(pair, carry):
        tiles = []
        for t in range(4):
            i = 2 * pair + t // 2
            if t % 2 == 0:
                s_re, s_im = sv[i, 0], sv[i, 1]
                made = [s_re * g_all[d] + s_im * g_turned[d] for d in range(chans)]
            parts = [made[d][4 * (t % 2) : 4 * (t % 2) + 4] for d in range(chans)]
            tile = jnp.concatenate(parts, axis=0)
            tiles.append(jnp.where(ch * 16 + i < reads, tile, 0.0))
        for b in range(4):
            low = jnp.zeros((16, LANES), jnp.float32)
            for t in range(4):
                shift = 32 * ((t - b) % 4)
                moved = pltpu.roll(tiles[t], shift, 1) if shift else tiles[t]
                low = jnp.where(lane16 // 32 == t, moved, low)
            zs[pl.ds(b, 16, stride=4), :] = low
        back_rows = zs[...].T
        for t in range(4):
            for p in range(2):
                at = 32 * t + 16 * p
                sgv[2 * pair + t // 2, pl.ds(2 * p + t % 2, 16, stride=4), :] = back_rows[at : at + 16]
        return carry

    with scope("weights_out"):
        lax.fori_loop(0, 8, weights_out, 0)
    passed_on(1)
    wait_bytes(red_far.at[2 * hubs - 1], rrecv.at[2])
    to_slab(-4, red_far.at[2 * hubs - 1], red_far.at[2 * hubs], rsend.at[1], rrecv.at[1])
    rows_back(1)
    last_own[...] = own_g[1]
    last_rx[...] = rx_g[1]
    wait_bytes(red_far.at[pl.ds(0, 2 * hubs)], rrecv.at[1])
    total = red_pair[3]
    for m in range(slabs // 4 - 1):
        total = total + red_far[m]
    gate_ref[...] = total[0:1, :16]
    bgrad_ref[...] = total[1:2, :16]
    for turn in range(2):
        wait_bytes(rx_anti.at[turn], ssend.at[turn, 0])
        wait_bytes(rx_near.at[turn], ssend.at[turn, 1])
        wait_bytes(tx_far.at[turn], ssend.at[turn, 2])
        wait_bytes(rx_modes.at[turn, pl.ds(0, 6 + 2 * hubs)], ssend.at[2 + turn, 0])
        wait_bytes(rx_modes.at[turn, pl.ds(0, 6 * hubs + 1)], ssend.at[2 + turn, 1])
        wait_bytes(rx_chan, csend.at[turn])
    wait_bytes(red_near, rsend.at[0])
    wait_bytes(red_far, rsend.at[1])


def column_synthesis(own, theirs, a, rows, tables):
    here = pl.ds(a * rows, rows)
    g = jnp.concatenate([own[here, :], theirs[here, :]], axis=1)
    block = (iota(g.shape, 1) & (LANES - 1)) // 32
    spread = jnp.concatenate([jnp.where(block == b, g, 0.0) for b in range(4)], axis=0)
    return dot3(split(spread), (tables[0][...], tables[1][...]))


def finish(
    rows, ov, gv, sgv, gate, bgrad, own, theirs, tth, ttl,
    out_hbm, fgrad_hbm, sgrad_hbm, gate_hbm, bgrad_hbm,
    fv, sem, fsem,
):
    pairs = ((ov, out_hbm), (sgv, sgrad_hbm), (gate, gate_hbm), (bgrad, bgrad_hbm))
    copies = [pltpu.make_async_copy(a, b, sem.at[n]) for n, (a, b) in enumerate(pairs)]
    for copy in copies:
        copy.start()
    chunk = 4 * rows
    for a in range(4):
        here = pl.ds(a * chunk, chunk)
        fv[here, :] = column_synthesis(own, theirs, a, rows, (tth, ttl)) + gv[here, :]
        copies.append(pltpu.make_async_copy(fv.at[here, :], fgrad_hbm.at[here, :], fsem.at[a]))
        copies[-1].start()
    for copy in copies:
        copy.wait()


def local(source_field, cotangent, spectral_weight, skip_gain, channel_bias, mode_limit, width_limit):
    channels, rows, cols = source_field.shape
    slabs, chans, modes = lax.axis_size("slab"), lax.axis_size("chan"), lax.axis_size("mode")
    outs = spectral_weight.shape[1]
    assert (channels, rows, modes, outs) == (16, 32, 2, 16 * chans)
    assert spectral_weight.shape[2:] == (16, 2, 2)
    flat = (channels * rows, cols)
    w = spectral_weight.transpose(0, 2, 3, 4, 1).reshape(channels, 64, outs)
    limits = mode_limit.T
    f32, bf16 = jnp.float32, jnp.bfloat16
    vmem, sems = pltpu.VMEM, pltpu.SemaphoreType.DMA
    hubs = slabs // 8 - 1
    assert slabs == 8 * (hubs + 1) and hubs > 0
    hbm_spec = pl.BlockSpec(memory_space=pltpu.HBM)
    vmem_spec = pl.BlockSpec(memory_space=pltpu.VMEM)
    square = (LANES, LANES)
    held = (
        (flat, f32), (flat, f32), (w.shape, f32), ((1, channels), f32), ((1, channels), f32),
        (square, f32), (square, f32), ((2 * LANES, cols), bf16), ((2 * LANES, cols), bf16),
    )
    found = pl.pallas_call(
        functools.partial(kernel, (slabs, chans, modes, rows, cols)),
        out_shape=tuple(jax.ShapeDtypeStruct(*h) for h in held),
        in_specs=[hbm_spec] * 7,
        out_specs=[vmem_spec] * len(held),
        scratch_shapes=[
            vmem(flat, f32), vmem(flat, f32), vmem(w.shape, f32),
            pltpu.SMEM(skip_gain.shape, f32), pltpu.SMEM(channel_bias.shape, f32),
            pltpu.SMEM(limits.shape, jnp.int32), pltpu.SMEM(width_limit.shape, jnp.int32),
            vmem((cols, 2 * LANES), bf16), vmem((cols, 2 * LANES), bf16),
            vmem((8 * slabs, 2 * LANES), bf16), vmem((8 * slabs, 2 * LANES), bf16),
            vmem((2 * LANES, 8 * slabs), bf16), vmem((2 * LANES, 8 * slabs), bf16),
            vmem((channels, chans, 8, LANES), f32), vmem((outs, LANES), f32),
            vmem((channels, 2, 8, LANES), f32),
            vmem(square, f32), vmem((2, *square), f32), vmem((2, *square), f32),
            vmem((2, slabs, 8, LANES), f32), vmem((2, 2, hubs + 1, 3, 8, LANES), f32),
            vmem((2, 8, LANES), f32),
            vmem((2, 2 * hubs, 8, LANES), f32), vmem((2, 2 * hubs, 8, LANES), f32),
            vmem((chans, 8, LANES), f32), vmem((chans - 1, 8, LANES), f32),
            vmem((2, slabs, 8, LANES), f32),
            vmem((2, *square), f32), vmem((2, *square), f32),
            vmem((chans, 8, LANES), f32), vmem((4, 2, LANES), f32),
            vmem((3, 2, LANES), f32), vmem((slabs // 4 - 1, 2, LANES), f32),
            sems((7,)), sems((5,)), sems((5,)), sems((4, 3)), sems((2, 3, hubs + 1)), sems((2,)),
            sems((2, hubs, 2)), sems((2,)), sems((2,)), sems((2,)), sems((2,)), sems((3,)),
        ],
        compiler_params=pltpu.CompilerParams(collective_id=0, has_side_effects=True, vmem_limit_bytes=40 << 20),
        name="fno_layer",
    )(
        *(
            pltpu.with_memory_space_constraint(a, pltpu.HBM)
            for a in (
                source_field.reshape(flat), cotangent.reshape(flat), w, skip_gain, channel_bias, limits, width_limit,
            )
        )
    )
    out, fgrad, sgrad, gate, bgrad = pl.pallas_call(
        functools.partial(finish, rows),
        out_shape=tuple(jax.ShapeDtypeStruct(*h) for h in held[:5]),
        in_specs=[vmem_spec] * len(held),
        out_specs=[hbm_spec] * 5,
        scratch_shapes=[vmem(flat, f32), pltpu.SemaphoreType.DMA((4,)), pltpu.SemaphoreType.DMA((4,))],
        compiler_params=pltpu.CompilerParams(vmem_limit_bytes=24 << 20),
        name="fno_finish",
    )(*found)
    sgrad = sgrad.reshape(channels, 16, 2, 2, outs).transpose(0, 4, 1, 2, 3)
    return (
        out.reshape(source_field.shape), fgrad.reshape(source_field.shape), sgrad,
        gate.reshape(channels), bgrad.reshape(channels),
    )


def solution(mesh):
    field = P(("member", "chan"), "slab", "mode")
    weight = P(("member", "chan"), None, "mode", None, "slab")
    channel = P(("member", "chan"))
    return jax.shard_map(
        local,
        mesh=mesh,
        in_specs=(field, field, weight, channel, channel, P("member", None), P("member")),
        out_specs=(field, field, weight, channel, channel),
        check_vma=False,
    )
```

```python
import functools
import math

import jax
import jax.numpy as jnp
from jax import lax
from jax.experimental import pallas as pl
from jax.experimental.pallas import tpu as pltpu
from jax.sharding import PartitionSpec as P

MESH = pl.DeviceIdType.MESH
LANES = 128
GELU_SLOPE = math.sqrt(2.0 / math.pi)
GELU_CUBE = 0.044715


def slab_offsets(slabs):
    hubs = slabs // 8 - 1
    far = [4 * m for m in range(1, hubs + 1)]
    found = [0, slabs // 2] + far + [-k for k in far]
    for sign in (1, -1):
        for j in range(1, 4):
            found += [sign * (j + 4 * m) for m in range(hubs + 1)]
    return found


def both_ways(ks):
    return [sign * k for k in ks for sign in (1, -1)]


def early_plan(slabs):
    top = slabs // 4
    hubs = [(top, slabs // 2 - top), (-top, slabs // 2 - top - 1), (4, top - 5), (-4, top - 5)]
    return hubs, [], both_ways((3, 2, 1))


def main_plan(slabs):
    half = slabs // 2
    hubs = [(k, half // 2 - 4 if abs(k) > 4 else 3) for k in both_ways((half // 2, 4))]
    first = [half] + both_ways(range(half - 1, half // 2 + half // 2 - 4, -1))
    return hubs, first, both_ways((3, 2, 1))


def offset_of(slot, slabs):
    hubs = slabs // 8 - 1
    first = 2 + 2 * hubs
    near = jnp.where(slot < 2 + hubs, 4 * (slot - 1), -4 * (slot - 1 - hubs))
    group, m = (slot - first) // (hubs + 1), (slot - first) % (hubs + 1)
    behind = jnp.where(group < 3, 1 + group + 4 * m, -(group - 2) - 4 * m)
    found = jnp.where(slot < first, near, behind)
    return jnp.where(slot == 0, 0, jnp.where(slot == 1, slabs // 2, found))


def split(x):
    high = x.astype(jnp.bfloat16)
    low = (x - high.astype(jnp.float32)).astype(jnp.bfloat16)
    return high, low


def dot3(a, b):
    (ah, al), (bh, bl) = a, b
    dot = functools.partial(jnp.dot, preferred_element_type=jnp.float32)
    return dot(ah, bh) + (dot(ah, bl) + dot(al, bh))


def sine(turns, extent):
    half, quarter = extent // 2, extent // 4
    t = ((turns + half) & (extent - 1)) - half
    t = jnp.where(t > quarter, half - t, jnp.where(t < -quarter, -half - t, t))
    v = t.astype(jnp.float32) * (2.0 * math.pi / extent)
    s = v * v
    poly = -2.5052108e-8
    for c in (2.7557319e-6, -1.9841270e-4, 8.3333333e-3, -1.6666667e-1, 1.0):
        poly = poly * s + c
    return poly * v


def iota(shape, dim):
    return lax.broadcasted_iota(jnp.int32, shape, dim)


def kernel(
    dims,
    x_hbm, cot_hbm, w_hbm, gain_hbm, bias_hbm, limit_hbm, width_hbm,
    ov, gv, sgv, gate_ref, bgrad_ref, last_own, last_rx, tth, ttl,
    xv, cv, wv, gain, bias, limit, width, tch, tcl, fh, fl, fth, ftl,
    wt, zs, sv,
    own_cols, tx_cols, rx_cols, tx_rows, rx_near, tx_far, rx_far, tx_chan, rx_chan, rx_modes,
    own_g, rx_g, g_chan, red_pair, red_near, red_far,
    lsem, msend, mrecv, ssend, nrecv, frecv, hrecv, arecv, csend, crecv, rsend, rrecv,
):
    slabs, chans, modes, rows, cols = dims
    chunk = 4 * rows
    me, ch, mo = lax.axis_index("slab"), lax.axis_index("chan"), lax.axis_index("mode")
    other = 1 - mo
    all_rows, all_cols = slabs * rows, modes * cols
    kx_count = 2 * slabs

    scope = jax.named_scope
    barrier = pltpu.get_barrier_semaphore()

    hubs = slabs // 8 - 1
    offsets = slab_offsets(slabs)
    partners = [k for k in offsets if 0 < abs(k) <= slabs // 4]
    early, main = early_plan(slabs), main_plan(slabs)

    def slot_of(k):
        k %= slabs
        return offsets.index(k - slabs if k > slabs // 2 else k)

    def slab_at(k):
        return {"slab": (me + k + slabs) & (slabs - 1)}

    with scope("greet"):
        for k in partners:
            pl.semaphore_signal(barrier, inc=1, device_id=slab_at(k), device_id_type=MESH)
    for k in range(1, chans):
        pl.semaphore_signal(barrier, inc=1, device_id={"chan": lax.rem(ch + k, chans)}, device_id_type=MESH)
    pl.semaphore_signal(barrier, inc=1, device_id={"mode": other}, device_id_type=MESH)

    pairs = (
        (x_hbm, xv), (cot_hbm, cv), (w_hbm, wv), (limit_hbm, limit), (width_hbm, width),
        (gain_hbm, gain), (bias_hbm, bias),
    )
    loads = [pltpu.make_async_copy(a, b, lsem.at[n]) for n, (a, b) in enumerate(pairs)]
    for load in loads:
        load.start()
    def to_mode(slot, src, dst):
        return pltpu.make_async_remote_copy(
            src_ref=src, dst_ref=dst, send_sem=msend.at[slot], recv_sem=mrecv.at[slot],
            device_id={"mode": other}, device_id_type=MESH,
        )

    def to_slab(k, src, dst, send_sem, recv_sem):
        pltpu.make_async_remote_copy(
            src_ref=src, dst_ref=dst, send_sem=send_sem, recv_sem=recv_sem,
            device_id=slab_at(k), device_id_type=MESH,
        ).start()

    def wait_bytes(ref, sem):
        pltpu.make_async_copy(ref, ref, sem).wait()

    lane = iota((8, LANES), 1)
    real_part = lane % 32 < 16

    def turned(v):
        re = iota(v.shape, 1) & 31 < 16
        return jnp.where(re, pltpu.roll(v, LANES - 16, 1), -pltpu.roll(v, 16, 1))

    def column_angles(n, w):
        holder = jnp.where(n < LANES, mo, other)
        freq = holder * 16 + (n & 15)
        cell = mo * cols + w
        return freq * cell + jnp.where(n & 31 < 16, all_cols // 4, all_cols // 2)

    with scope("column_table"):
        shape = (cols, 2 * LANES)
        tch[...], tcl[...] = split(sine(column_angles(iota(shape, 1), iota(shape, 0)), all_cols))

    def row_angles(k, n):
        kx = 2 * ((me + offset_of(k >> 3, slabs) + slabs) & (slabs - 1)) + ((k >> 2) & 1)
        kx = jnp.where(kx < kx_count // 2, kx, kx + all_rows - kx_count)
        half = LANES
        cell = me * rows + (n & (rows - 1))
        angle = kx * cell + jnp.where(n < half, all_rows // 4, 0)
        same = (k & 3) == ((n & (half - 1)) // rows)
        return jnp.where(same, sine(angle, all_rows), 0.0)

    def column_forward(a, values):
        d = dot3(split(values), (tch[...], tcl[...]))
        block = (iota((rows, 2 * LANES), 1) % LANES) // 32
        packed = d[:rows]
        for b in range(1, 4):
            packed = jnp.where(block == b, d[b * rows : (b + 1) * rows], packed)
        own_cols[pl.ds(a * rows, rows), :] = packed[:, :LANES]
        return packed[:, LANES:]

    with scope("row_table"):
        shape = (8 * slabs, 2 * LANES)
        fh[...], fl[...] = split(row_angles(iota(shape, 0), iota(shape, 1)))

    with scope("load_wait"):
        loads[0].wait()

    def first_chunk(a, carry):
        values = xv[pl.ds(a * chunk, chunk), :]
        tx_cols[0, pl.ds(a * rows, rows), :] = column_forward(a, values)
        return carry

    with scope("first_columns"):
        lax.fori_loop(0, 4, first_chunk, 0, unroll=True)
    with scope("barrier_wait"):
        pl.semaphore_wait(barrier, len(partners) + chans - 1 + 1)

    def rows_forward(turn):
        copy = to_mode(turn, tx_cols.at[turn], rx_cols.at[turn])
        copy.start()
        with scope("columns_pair"):
            copy.wait()
        with scope("rows_dot"):
            lined = own_cols[...] + rx_cols[turn]
            both = jnp.concatenate([lined, turned(lined)], axis=0)
            partial = dot3((fh[...], fl[...]), split(both))
            tx_rows[turn] = partial.reshape(slabs, 8, LANES)
        with scope("rows_send"):
            chain, first, last = main if turn else early

            def near(n):
                k, reach = chain[n]
                for j in range(reach, 0, -1):
                    step = j if k > 0 else -j
                    to_slab(
                        step, tx_rows.at[turn, slot_of(k + step)], rx_near.at[turn, n, j - 1],
                        ssend.at[turn, 1], nrecv.at[turn, n],
                    )

            def direct(ks, at):
                for n, k in enumerate(ks):
                    to_slab(k, tx_rows.at[turn, slot_of(k)], rx_far.at[turn, at + n], ssend.at[turn, 0], frecv.at[turn])

            near(0)
            near(1)
            direct(first, len(chain))
            for n in range(2, len(chain)):
                near(n)
            direct(last, len(chain) + len(first))

    def owned(turn):
        chain, first, last = main if turn else early
        for n, (k, reach) in enumerate(chain):
            with scope("near_wait"):
                wait_bytes(rx_near.at[turn, n, pl.ds(0, reach)], nrecv.at[turn, n])
            total = tx_rows[turn, slot_of(k)]
            for j in range(reach):
                total = total + rx_near[turn, n, j]
            tx_far[turn, n] = total
            to_slab(k, tx_far.at[turn, n], rx_far.at[turn, n], ssend.at[turn, 2], frecv.at[turn])
        if turn:
            with scope("sums_near"):
                wait_bytes(red_near, rrecv.at[0])
                total = red_pair[2]
                for j in range(3):
                    total = total + red_near[j]
                red_pair[3] = total
                for m in range(1, slabs // 4):
                    to_slab(4 * m, red_pair.at[3], red_far.at[m - 1], rsend.at[1], rrecv.at[1])
        count = len(chain) + len(first) + len(last)
        with scope("rows_wait"):
            wait_bytes(rx_far.at[turn, pl.ds(0, count)], frecv.at[turn])
        total = tx_rows[turn, 0]
        for n in range(count):
            total = total + rx_far[turn, n]
        return total

    rows_forward(0)

    with scope("back_tables"):
        shape = (2 * LANES, cols)
        tth[...], ttl[...] = split(sine(column_angles(iota(shape, 0), iota(shape, 1)), all_cols))
        shape = (2 * LANES, 8 * slabs)
        fth[...], ftl[...] = split(row_angles(iota(shape, 1), iota(shape, 0)))

    for load in loads[3:]:
        load.wait()
    sub = iota((8, LANES), 0)
    keep_col = jnp.zeros((8, LANES), jnp.int32)
    keep_row = jnp.zeros((8, LANES), jnp.int32)
    for c in range(16):
        here = (sub % 4 == c // 4) & (lane // 32 == c % 4)
        keep_col = jnp.where(here, limit[0, ch * 16 + c], keep_col)
        keep_row = jnp.where(here, limit[1, ch * 16 + c], keep_row)
    col_freq = mo * 16 + lane % 16
    row_freq = me * 2 + sub // 4
    kept = (col_freq < keep_col) & ((row_freq < keep_row) | (kx_count - row_freq < keep_row))
    scale = jnp.where(col_freq == 0, 1.0, 2.0) / (all_rows * all_cols)
    weights = jnp.where(kept, scale, 0.0)

    sub16 = iota((16, LANES), 0)
    lane16 = iota((16, LANES), 1)
    reads = jnp.zeros((16, LANES), jnp.int32)
    for o in range(16 * chans):
        reads = jnp.where((sub16 == o // 4) & (lane16 // 32 == o % 4), width[o], reads)

    loads[2].wait()

    def weights_in(pair, carry):
        parts = []
        for t in range(4):
            for p in range(2):
                parts.append(wv[2 * pair + t // 2, pl.ds(2 * p + t % 2, 16, stride=4), :])
        zs[...] = jnp.concatenate(parts, axis=0).T
        by_low = [zs[pl.ds(b, 16, stride=4), :] for b in range(4)]
        for t in range(4):
            i = 2 * pair + t // 2
            tile = jnp.zeros((16, LANES), jnp.float32)
            for b in range(4):
                shift = 32 * ((b - t) % 4)
                moved = pltpu.roll(by_low[b], shift, 1) if shift else by_low[b]
                tile = jnp.where(lane16 // 32 == b, moved, tile)
            tile = jnp.where(ch * 16 + i < reads, tile, 0.0)
            for d in range(chans):
                wt[i, d, pl.ds(4 * (t % 2), 4), :] = tile[4 * d : 4 * d + 4]
        return carry

    with jax.named_scope("weights_in"):
        lax.fori_loop(0, 8, weights_in, 0)

    spectra = owned(0)
    for a in range(4):
        e = jnp.where(
            sub < 4,
            jnp.broadcast_to(spectra[a : a + 1], (8, LANES)),
            jnp.broadcast_to(spectra[4 + a : 5 + a], (8, LANES)),
        )
        rolled = [e] + [pltpu.roll(e, 16 * m, 1) for m in range(1, 8)]
        for q in range(8):
            copies = rolled[(0 - q) % 8]
            for t in range(1, 8):
                copies = jnp.where(lane // 16 == t, rolled[(t - q) % 8], copies)
            sv[4 * a + q // 2, q % 2] = copies

    zero = jnp.zeros((8, LANES), jnp.float32)

    def contract(i, sums):
        s_re, s_im = sv[i, 0], sv[i, 1]
        first = tuple(sums[d] + s_re * wt[i, d] for d in range(chans))
        second = tuple(sums[chans + d] + s_im * wt[i, d] for d in range(chans))
        return first + second

    sums = lax.fori_loop(0, 16, contract, (zero,) * (2 * chans), unroll=4)
    for d in range(chans):
        tx_chan[d] = sums[d] - turned(sums[chans + d])

    def to_chan(slot, k, src, dst):
        return pltpu.make_async_remote_copy(
            src_ref=src, dst_ref=dst, send_sem=csend.at[slot], recv_sem=crecv.at[slot],
            device_id={"chan": lax.rem(ch + k, chans)}, device_id_type=MESH,
        )

    for k in range(1, chans):
        to_chan(0, k, tx_chan.at[lax.rem(ch + k, chans)], rx_chan.at[chans - 1 - k]).start()
    with scope("chan_wait"):
        wait_bytes(rx_chan, crecv.at[0])
    modes_out = tx_chan[ch]
    for k in range(chans - 1):
        modes_out = modes_out + rx_chan[k]

    def everywhere(turn, tile):
        rx = rx_modes.at[turn]
        rx[0] = tile
        with scope("modes_send"):
            chain, first, last = main
            order = [k for k, _ in chain[:2]] + first + [k for k, _ in chain[2:]] + last
            kinds = [k for k, _ in chain]
            for k in order:
                sem = hrecv.at[turn, kinds.index(k)] if k in kinds else arecv.at[turn]
                to_slab(k, rx.at[0], rx.at[slot_of(-k)], ssend.at[2 + turn, 0], sem)

    def passed_on(turn):
        rx = rx_modes.at[turn]
        chain = main[0]
        for n in list(range(2, len(chain))) + [0, 1]:
            k, reach = chain[n]
            held = rx.at[slot_of(-k)]
            with scope("hub_wait"):
                wait_bytes(held, hrecv.at[turn, n])
            for j in range(reach, 0, -1):
                step = j if k > 0 else -j
                to_slab(step, held, rx.at[slot_of(-k - step)], ssend.at[2 + turn, 1], arecv.at[turn])

    def rows_back(turn):
        with scope("modes_wait"):
            wait_bytes(rx_modes.at[turn, pl.ds(0, slabs - 1 - len(main[0]))], arecv.at[turn])
        with scope("back_dot"):
            found = rx_modes[turn].reshape(8 * slabs, LANES)
            both = dot3((fth[...], ftl[...]), split(found))
            own_g[turn] = both[:LANES] - turned(both[LANES:])
        with scope("back_pair"):
            copy = to_mode(2 + turn, own_g.at[turn], rx_g.at[turn])
            copy.start()
            copy.wait()

    everywhere(0, modes_out * weights)
    loads[1].wait()
    passed_on(0)
    rows_back(0)

    def gelu_chunk(a, carry):
        gates, biases = carry
        branch = column_synthesis(own_g.at[0], rx_g.at[0], a, rows, (tth, ttl))
        grads = []
        for b in range(4):
            c = 4 * a + b
            here = pl.ds(c * rows, rows)
            x = xv[here, :]
            v = branch[b * rows : (b + 1) * rows] + gain[c] * x + bias[c]
            v2 = v * v
            t = jnp.tanh(GELU_SLOPE * (v + GELU_CUBE * (v2 * v)))
            cdf = 0.5 * (1.0 + t)
            ov[here, :] = v * cdf
            slope = cdf + (0.5 * GELU_SLOPE) * (v * (1.0 - t * t)) * (1.0 + (3.0 * GELU_CUBE) * v2)
            grad = cv[here, :] * slope
            gv[here, :] = gain[c] * grad
            grads.append(grad)
            gate = jnp.sum(jnp.sum(grad * x, axis=0, keepdims=True), axis=1, keepdims=True)
            plain = jnp.sum(jnp.sum(grad, axis=0, keepdims=True), axis=1, keepdims=True)
            spot = iota((1, LANES), 1) == c
            gates = jnp.where(spot, gate, gates)
            biases = jnp.where(spot, plain, biases)
        tx_cols[1, pl.ds(a * rows, rows), :] = column_forward(a, jnp.concatenate(grads, axis=0))
        return gates, biases

    empty = jnp.zeros((1, LANES), jnp.float32)
    with scope("gelu"):
        gates, biases = lax.fori_loop(0, 4, gelu_chunk, (empty, empty), unroll=True)
    rows_forward(1)

    red_pair[0] = jnp.concatenate([gates, biases], axis=0)
    with scope("pair_sums"):
        copy = to_mode(4, red_pair.at[0], red_pair.at[1])
        copy.start()
        copy.wait()
        red_pair[2] = red_pair[0] + red_pair[1]
        for j in range(1, 4):
            pltpu.make_async_remote_copy(
                src_ref=red_pair.at[2], dst_ref=red_near.at[j - 1], send_sem=rsend.at[0], recv_sem=rrecv.at[0],
                device_id={"slab": me ^ j}, device_id_type=MESH,
            ).start()

    g_chan[ch] = owned(1) * weights
    for k in range(1, chans):
        to_chan(1, k, g_chan.at[ch], g_chan.at[ch]).start()
    with scope("chan_wait_two"):
        wait_bytes(g_chan.at[pl.ds(0, chans - 1)], crecv.at[1])
    g_all = [g_chan[d] for d in range(chans)]
    g_turned = [turned(g) for g in g_all]

    def contract_back(i):
        first, second = zero, zero
        for d in range(chans):
            w = wt[i, d]
            first = first + w * g_all[d]
            second = second + w * g_turned[d]
        v = jnp.where(real_part, first + pltpu.roll(first, 16, 1), second + pltpu.roll(second, 16, 1))
        v = v + pltpu.roll(v, 32, 1)
        return v + pltpu.roll(v, 64, 1)

    back = zero
    for a in range(4):
        m = contract_back(4 * a)
        for b in range(1, 4):
            m = jnp.where(lane // 32 == b, contract_back(4 * a + b), m)
        for x in range(2):
            row = jnp.sum(m[4 * x : 4 * x + 4], axis=0, keepdims=True)
            back = jnp.where(sub == 4 * x + a, jnp.broadcast_to(row, (8, LANES)), back)
    everywhere(1, back)

    def weights_out(pair, carry):
        tiles = []
        for t in range(4):
            i = 2 * pair + t // 2
            if t % 2 == 0:
                s_re, s_im = sv[i, 0], sv[i, 1]
                made = [s_re * g_all[d] + s_im * g_turned[d] for d in range(chans)]
            parts = [made[d][4 * (t % 2) : 4 * (t % 2) + 4] for d in range(chans)]
            tile = jnp.concatenate(parts, axis=0)
            tiles.append(jnp.where(ch * 16 + i < reads, tile, 0.0))
        for b in range(4):
            low = jnp.zeros((16, LANES), jnp.float32)
            for t in range(4):
                shift = 32 * ((t - b) % 4)
                moved = pltpu.roll(tiles[t], shift, 1) if shift else tiles[t]
                low = jnp.where(lane16 // 32 == t, moved, low)
            zs[pl.ds(b, 16, stride=4), :] = low
        back_rows = zs[...].T
        for t in range(4):
            for p in range(2):
                at = 32 * t + 16 * p
                sgv[2 * pair + t // 2, pl.ds(2 * p + t % 2, 16, stride=4), :] = back_rows[at : at + 16]
        return carry

    with scope("weights_out"):
        lax.fori_loop(0, 8, weights_out, 0)
    passed_on(1)
    rows_back(1)
    last_own[...] = own_g[1]
    last_rx[...] = rx_g[1]
    wait_bytes(red_far, rrecv.at[1])
    total = red_pair[3]
    for m in range(slabs // 4 - 1):
        total = total + red_far[m]
    gate_ref[...] = total[0:1, :16]
    bgrad_ref[...] = total[1:2, :16]
    for turn in range(2):
        chain, first, last = main if turn else early
        wait_bytes(rx_far.at[turn, pl.ds(0, len(first) + len(last))], ssend.at[turn, 0])
        wait_bytes(tx_rows.at[turn, pl.ds(0, sum(reach for _, reach in chain))], ssend.at[turn, 1])
        wait_bytes(tx_far.at[turn, pl.ds(0, len(chain))], ssend.at[turn, 2])
        passed = sum(reach for _, reach in main[0])
        wait_bytes(rx_modes.at[turn, pl.ds(0, slabs - 1 - passed)], ssend.at[2 + turn, 0])
        wait_bytes(rx_modes.at[turn, pl.ds(0, passed)], ssend.at[2 + turn, 1])
        wait_bytes(rx_chan, csend.at[turn])
    wait_bytes(red_near, rsend.at[0])
    wait_bytes(red_far, rsend.at[1])


def column_synthesis(own, theirs, a, rows, tables):
    here = pl.ds(a * rows, rows)
    g = jnp.concatenate([own[here, :], theirs[here, :]], axis=1)
    block = (iota(g.shape, 1) & (LANES - 1)) // 32
    spread = jnp.concatenate([jnp.where(block == b, g, 0.0) for b in range(4)], axis=0)
    return dot3(split(spread), (tables[0][...], tables[1][...]))


def finish(
    rows, ov, gv, sgv, gate, bgrad, own, theirs, tth, ttl,
    out_hbm, fgrad_hbm, sgrad_hbm, gate_hbm, bgrad_hbm,
    fv, sem, fsem,
):
    pairs = ((ov, out_hbm), (sgv, sgrad_hbm), (gate, gate_hbm), (bgrad, bgrad_hbm))
    copies = [pltpu.make_async_copy(a, b, sem.at[n]) for n, (a, b) in enumerate(pairs)]
    for copy in copies:
        copy.start()
    chunk = 4 * rows
    for a in range(4):
        here = pl.ds(a * chunk, chunk)
        fv[here, :] = column_synthesis(own, theirs, a, rows, (tth, ttl)) + gv[here, :]
        copies.append(pltpu.make_async_copy(fv.at[here, :], fgrad_hbm.at[here, :], fsem.at[a]))
        copies[-1].start()
    for copy in copies:
        copy.wait()


def local(source_field, cotangent, spectral_weight, skip_gain, channel_bias, mode_limit, width_limit):
    channels, rows, cols = source_field.shape
    slabs, chans, modes = lax.axis_size("slab"), lax.axis_size("chan"), lax.axis_size("mode")
    outs = spectral_weight.shape[1]
    assert (channels, rows, modes, outs) == (16, 32, 2, 16 * chans)
    assert spectral_weight.shape[2:] == (16, 2, 2)
    flat = (channels * rows, cols)
    w = spectral_weight.transpose(0, 2, 3, 4, 1).reshape(channels, 64, outs)
    limits = mode_limit.T
    f32, bf16 = jnp.float32, jnp.bfloat16
    vmem, sems = pltpu.VMEM, pltpu.SemaphoreType.DMA
    hubs = slabs // 8 - 1
    plans = early_plan(slabs), main_plan(slabs)
    chains = max(len(p[0]) for p in plans)
    arrivals = max(sum(map(len, p)) for p in plans)
    reach = max(r for p in plans for _, r in p[0])
    assert all(sum(r for _, r in p[0]) + sum(map(len, p)) == slabs - 1 for p in plans)
    hbm_spec = pl.BlockSpec(memory_space=pltpu.HBM)
    vmem_spec = pl.BlockSpec(memory_space=pltpu.VMEM)
    square = (LANES, LANES)
    held = (
        (flat, f32), (flat, f32), (w.shape, f32), ((1, channels), f32), ((1, channels), f32),
        (square, f32), (square, f32), ((2 * LANES, cols), bf16), ((2 * LANES, cols), bf16),
    )
    found = pl.pallas_call(
        functools.partial(kernel, (slabs, chans, modes, rows, cols)),
        out_shape=tuple(jax.ShapeDtypeStruct(*h) for h in held),
        in_specs=[hbm_spec] * 7,
        out_specs=[vmem_spec] * len(held),
        scratch_shapes=[
            vmem(flat, f32), vmem(flat, f32), vmem(w.shape, f32),
            pltpu.SMEM(skip_gain.shape, f32), pltpu.SMEM(channel_bias.shape, f32),
            pltpu.SMEM(limits.shape, jnp.int32), pltpu.SMEM(width_limit.shape, jnp.int32),
            vmem((cols, 2 * LANES), bf16), vmem((cols, 2 * LANES), bf16),
            vmem((8 * slabs, 2 * LANES), bf16), vmem((8 * slabs, 2 * LANES), bf16),
            vmem((2 * LANES, 8 * slabs), bf16), vmem((2 * LANES, 8 * slabs), bf16),
            vmem((channels, chans, 8, LANES), f32), vmem((outs, LANES), f32),
            vmem((channels, 2, 8, LANES), f32),
            vmem(square, f32), vmem((2, *square), f32), vmem((2, *square), f32),
            vmem((2, slabs, 8, LANES), f32), vmem((2, chains, reach, 8, LANES), f32),
            vmem((2, chains, 8, LANES), f32), vmem((2, arrivals, 8, LANES), f32),
            vmem((chans, 8, LANES), f32), vmem((chans - 1, 8, LANES), f32),
            vmem((2, slabs, 8, LANES), f32),
            vmem((2, *square), f32), vmem((2, *square), f32),
            vmem((chans, 8, LANES), f32), vmem((4, 2, LANES), f32),
            vmem((3, 2, LANES), f32), vmem((slabs // 4 - 1, 2, LANES), f32),
            sems((7,)), sems((5,)), sems((5,)), sems((4, 3)), sems((2, chains)), sems((2,)),
            sems((2, chains)), sems((2,)), sems((2,)), sems((2,)), sems((2,)), sems((2,)),
        ],
        compiler_params=pltpu.CompilerParams(collective_id=0, has_side_effects=True, vmem_limit_bytes=40 << 20),
        name="fno_layer",
    )(
        *(
            pltpu.with_memory_space_constraint(a, pltpu.HBM)
            for a in (
                source_field.reshape(flat), cotangent.reshape(flat), w, skip_gain, channel_bias, limits, width_limit,
            )
        )
    )
    out, fgrad, sgrad, gate, bgrad = pl.pallas_call(
        functools.partial(finish, rows),
        out_shape=tuple(jax.ShapeDtypeStruct(*h) for h in held[:5]),
        in_specs=[vmem_spec] * len(held),
        out_specs=[hbm_spec] * 5,
        scratch_shapes=[vmem(flat, f32), pltpu.SemaphoreType.DMA((4,)), pltpu.SemaphoreType.DMA((4,))],
        compiler_params=pltpu.CompilerParams(vmem_limit_bytes=24 << 20),
        name="fno_finish",
    )(*found)
    sgrad = sgrad.reshape(channels, 16, 2, 2, outs).transpose(0, 4, 1, 2, 3)
    return (
        out.reshape(source_field.shape), fgrad.reshape(source_field.shape), sgrad,
        gate.reshape(channels), bgrad.reshape(channels),
    )


def solution(mesh):
    field = P(("member", "chan"), "slab", "mode")
    weight = P(("member", "chan"), None, "mode", None, "slab")
    channel = P(("member", "chan"))
    return jax.shard_map(
        local,
        mesh=mesh,
        in_specs=(field, field, weight, channel, channel, P("member", None), P("member")),
        out_specs=(field, field, weight, channel, channel),
        check_vma=False,
    )
```

```python
import functools
import math

import jax
import jax.numpy as jnp
from jax import lax
from jax.experimental import pallas as pl
from jax.experimental.pallas import tpu as pltpu
from jax.sharding import PartitionSpec as P

MESH = pl.DeviceIdType.MESH
LANES = 128
GELU_SLOPE = math.sqrt(2.0 / math.pi)
GELU_CUBE = 0.044715


def slab_offsets(slabs):
    hubs = slabs // 8 - 1
    far = [4 * m for m in range(1, hubs + 1)]
    found = [0, slabs // 2] + far + [-k for k in far]
    for sign in (1, -1):
        for j in range(1, 4):
            found += [sign * (j + 4 * m) for m in range(hubs + 1)]
    return found


def both_ways(ks):
    return [sign * k for k in ks for sign in (1, -1)]


def early_plan(slabs):
    top = slabs // 4
    hubs = [(top, slabs // 2 - top), (-top, slabs // 2 - top - 1), (4, top - 5), (-4, top - 5)]
    return hubs, [], both_ways((3, 2, 1))


def main_plans(slabs):
    half = slabs // 2
    hubs = [(k, half // 2 - 4 if abs(k) > 4 else 3) for k in both_ways((half // 2, 4))]
    first = [half] + both_ways(range(half - 1, half - 4, -1))
    many = [(k, 3) for k in both_ways(range(half - 4, 0, -4))]
    return (hubs, first, both_ways((3, 2, 1))), (many, [half], both_ways((3, 2, 1)))


def offset_of(slot, slabs):
    hubs = slabs // 8 - 1
    first = 2 + 2 * hubs
    near = jnp.where(slot < 2 + hubs, 4 * (slot - 1), -4 * (slot - 1 - hubs))
    group, m = (slot - first) // (hubs + 1), (slot - first) % (hubs + 1)
    behind = jnp.where(group < 3, 1 + group + 4 * m, -(group - 2) - 4 * m)
    found = jnp.where(slot < first, near, behind)
    return jnp.where(slot == 0, 0, jnp.where(slot == 1, slabs // 2, found))


def split(x):
    high = x.astype(jnp.bfloat16)
    low = (x - high.astype(jnp.float32)).astype(jnp.bfloat16)
    return high, low


def dot3(a, b):
    (ah, al), (bh, bl) = a, b
    dot = functools.partial(jnp.dot, preferred_element_type=jnp.float32)
    return dot(ah, bh) + (dot(ah, bl) + dot(al, bh))


def sine(turns, extent):
    half, quarter = extent // 2, extent // 4
    t = ((turns + half) & (extent - 1)) - half
    t = jnp.where(t > quarter, half - t, jnp.where(t < -quarter, -half - t, t))
    v = t.astype(jnp.float32) * (2.0 * math.pi / extent)
    s = v * v
    poly = -2.5052108e-8
    for c in (2.7557319e-6, -1.9841270e-4, 8.3333333e-3, -1.6666667e-1, 1.0):
        poly = poly * s + c
    return poly * v


def iota(shape, dim):
    return lax.broadcasted_iota(jnp.int32, shape, dim)


def kernel(
    dims,
    x_hbm, cot_hbm, w_hbm, gain_hbm, bias_hbm, limit_hbm, width_hbm,
    ov, gv, sgv, gate_ref, bgrad_ref, last_own, last_rx, tth, ttl,
    xv, cv, wv, gain, bias, limit, width, tch, tcl, fh, fl, fth, ftl,
    wt, zs, sv,
    own_cols, tx_cols, rx_cols, tx_rows, rx_near, tx_far, rx_far, tx_chan, rx_chan, rx_modes, mine,
    own_g, rx_g, g_chan, red_pair, red_near, red_far,
    lsem, msend, mrecv, ssend, nrecv, frecv, hrecv, arecv, csend, crecv, rsend, rrecv,
):
    slabs, chans, modes, rows, cols = dims
    chunk = 4 * rows
    me, ch, mo = lax.axis_index("slab"), lax.axis_index("chan"), lax.axis_index("mode")
    other = 1 - mo
    all_rows, all_cols = slabs * rows, modes * cols
    kx_count = 2 * slabs

    scope = jax.named_scope
    barrier = pltpu.get_barrier_semaphore()

    hubs = slabs // 8 - 1
    offsets = slab_offsets(slabs)
    partners = sorted((k for k in offsets if 0 < abs(k) <= slabs // 4), key=lambda k: -abs(k))
    early, mains = early_plan(slabs), main_plans(slabs)

    def by_core(f):
        for core, plan in enumerate(mains):
            pl.when(mo == core)(functools.partial(f, plan))

    def slot_of(k):
        k %= slabs
        return offsets.index(k - slabs if k > slabs // 2 else k)

    def slab_at(k):
        return {"slab": (me + k + slabs) & (slabs - 1)}

    with scope("greet"):
        for k in partners:
            pl.semaphore_signal(barrier, inc=1, device_id=slab_at(k), device_id_type=MESH)
    for k in range(1, chans):
        pl.semaphore_signal(barrier, inc=1, device_id={"chan": lax.rem(ch + k, chans)}, device_id_type=MESH)
    pl.semaphore_signal(barrier, inc=1, device_id={"mode": other}, device_id_type=MESH)

    pairs = (
        (x_hbm, xv), (cot_hbm, cv), (w_hbm, wv), (limit_hbm, limit), (width_hbm, width),
        (gain_hbm, gain), (bias_hbm, bias),
    )
    loads = [pltpu.make_async_copy(a, b, lsem.at[n]) for n, (a, b) in enumerate(pairs)]
    for load in loads:
        load.start()
    def to_mode(slot, src, dst):
        return pltpu.make_async_remote_copy(
            src_ref=src, dst_ref=dst, send_sem=msend.at[slot], recv_sem=mrecv.at[slot],
            device_id={"mode": other}, device_id_type=MESH,
        )

    def to_slab(k, src, dst, send_sem, recv_sem):
        pltpu.make_async_remote_copy(
            src_ref=src, dst_ref=dst, send_sem=send_sem, recv_sem=recv_sem,
            device_id=slab_at(k), device_id_type=MESH,
        ).start()

    def wait_bytes(ref, sem):
        pltpu.make_async_copy(ref, ref, sem).wait()

    lane = iota((8, LANES), 1)
    real_part = lane % 32 < 16

    def turned(v):
        re = iota(v.shape, 1) & 31 < 16
        return jnp.where(re, pltpu.roll(v, LANES - 16, 1), -pltpu.roll(v, 16, 1))

    def column_angles(n, w):
        holder = jnp.where(n < LANES, mo, other)
        freq = holder * 16 + (n & 15)
        cell = mo * cols + w
        return freq * cell + jnp.where(n & 31 < 16, all_cols // 4, all_cols // 2)

    with scope("column_table"):
        shape = (cols, 2 * LANES)
        tch[...], tcl[...] = split(sine(column_angles(iota(shape, 1), iota(shape, 0)), all_cols))

    def row_angles(k, n):
        kx = 2 * ((me + offset_of(k >> 3, slabs) + slabs) & (slabs - 1)) + ((k >> 2) & 1)
        kx = jnp.where(kx < kx_count // 2, kx, kx + all_rows - kx_count)
        half = LANES
        cell = me * rows + (n & (rows - 1))
        angle = kx * cell + jnp.where(n < half, all_rows // 4, 0)
        same = (k & 3) == ((n & (half - 1)) // rows)
        return jnp.where(same, sine(angle, all_rows), 0.0)

    def column_forward(a, values):
        d = dot3(split(values), (tch[...], tcl[...]))
        block = (iota((rows, 2 * LANES), 1) % LANES) // 32
        packed = d[:rows]
        for b in range(1, 4):
            packed = jnp.where(block == b, d[b * rows : (b + 1) * rows], packed)
        own_cols[pl.ds(a * rows, rows), :] = packed[:, :LANES]
        return packed[:, LANES:]

    with scope("row_table"):
        shape = (8 * slabs, 2 * LANES)
        fh[...], fl[...] = split(row_angles(iota(shape, 0), iota(shape, 1)))

    with scope("load_wait"):
        loads[0].wait()

    def first_chunk(a, carry):
        values = xv[pl.ds(a * chunk, chunk), :]
        tx_cols[0, pl.ds(a * rows, rows), :] = column_forward(a, values)
        return carry

    with scope("first_columns"):
        lax.fori_loop(0, 4, first_chunk, 0, unroll=True)
    with scope("barrier_wait"):
        pl.semaphore_wait(barrier, len(partners) + chans - 1 + 1)

    def rows_forward(turn):
        copy = to_mode(turn, tx_cols.at[turn], rx_cols.at[turn])
        copy.start()
        with scope("columns_pair"):
            copy.wait()
        with scope("rows_dot"):
            lined = own_cols[...] + rx_cols[turn]
            both = jnp.concatenate([lined, turned(lined)], axis=0)
            partial = dot3((fh[...], fl[...]), split(both))
            tx_rows[turn] = partial.reshape(slabs, 8, LANES)
        def send(plan):
            chain, first, last = plan

            def near(n):
                k, reach = chain[n]
                for j in range(reach, 0, -1):
                    step = j if k > 0 else -j
                    to_slab(
                        step, tx_rows.at[turn, slot_of(k + step)], rx_near.at[turn, n, j - 1],
                        ssend.at[turn, 1], nrecv.at[turn, n],
                    )

            def direct(ks, at):
                for n, k in enumerate(ks):
                    to_slab(k, tx_rows.at[turn, slot_of(k)], rx_far.at[turn, at + n], ssend.at[turn, 0], frecv.at[turn])

            near(0)
            near(1)
            direct(first, len(chain))
            for n in range(2, len(chain)):
                near(n)
            direct(last, len(chain) + len(first))

        with scope("rows_send"):
            by_core(send) if turn else send(early)

    def hub_sums(turn, plan):
        for n, (k, reach) in enumerate(plan[0]):
            with scope("near_wait"):
                wait_bytes(rx_near.at[turn, n, pl.ds(0, reach)], nrecv.at[turn, n])
            total = tx_rows[turn, slot_of(k)]
            for j in range(reach):
                total = total + rx_near[turn, n, j]
            tx_far[turn, n] = total
            to_slab(k, tx_far.at[turn, n], rx_far.at[turn, n], ssend.at[turn, 2], frecv.at[turn])
    def near_sums():
        with scope("sums_near"):
            wait_bytes(red_near, rrecv.at[0])
            total = red_pair[2]
            for j in range(3):
                total = total + red_near[j]
            red_pair[3] = total
            for m in range(1, slabs // 4):
                to_slab(4 * m, red_pair.at[3], red_far.at[m - 1], rsend.at[1], rrecv.at[1])

    def owned(turn, plan):
        count = sum(map(len, plan))
        with scope("rows_wait"):
            wait_bytes(rx_far.at[turn, pl.ds(0, count)], frecv.at[turn])
        total = tx_rows[turn, 0]
        for n in range(count):
            total = total + rx_far[turn, n]
        mine[...] = total

    rows_forward(0)
    hub_sums(0, early)

    with scope("back_tables"):
        shape = (2 * LANES, cols)
        tth[...], ttl[...] = split(sine(column_angles(iota(shape, 0), iota(shape, 1)), all_cols))
        shape = (2 * LANES, 8 * slabs)
        fth[...], ftl[...] = split(row_angles(iota(shape, 1), iota(shape, 0)))

    for load in loads[3:]:
        load.wait()
    sub = iota((8, LANES), 0)
    keep_col = jnp.zeros((8, LANES), jnp.int32)
    keep_row = jnp.zeros((8, LANES), jnp.int32)
    for c in range(16):
        here = (sub % 4 == c // 4) & (lane // 32 == c % 4)
        keep_col = jnp.where(here, limit[0, ch * 16 + c], keep_col)
        keep_row = jnp.where(here, limit[1, ch * 16 + c], keep_row)
    col_freq = mo * 16 + lane % 16
    row_freq = me * 2 + sub // 4
    kept = (col_freq < keep_col) & ((row_freq < keep_row) | (kx_count - row_freq < keep_row))
    scale = jnp.where(col_freq == 0, 1.0, 2.0) / (all_rows * all_cols)
    weights = jnp.where(kept, scale, 0.0)

    sub16 = iota((16, LANES), 0)
    lane16 = iota((16, LANES), 1)
    reads = jnp.zeros((16, LANES), jnp.int32)
    for o in range(16 * chans):
        reads = jnp.where((sub16 == o // 4) & (lane16 // 32 == o % 4), width[o], reads)

    loads[2].wait()

    def weights_in(pair, carry):
        parts = []
        for t in range(4):
            for p in range(2):
                parts.append(wv[2 * pair + t // 2, pl.ds(2 * p + t % 2, 16, stride=4), :])
        zs[...] = jnp.concatenate(parts, axis=0).T
        by_low = [zs[pl.ds(b, 16, stride=4), :] for b in range(4)]
        for t in range(4):
            i = 2 * pair + t // 2
            tile = jnp.zeros((16, LANES), jnp.float32)
            for b in range(4):
                shift = 32 * ((b - t) % 4)
                moved = pltpu.roll(by_low[b], shift, 1) if shift else by_low[b]
                tile = jnp.where(lane16 // 32 == b, moved, tile)
            tile = jnp.where(ch * 16 + i < reads, tile, 0.0)
            for d in range(chans):
                wt[i, d, pl.ds(4 * (t % 2), 4), :] = tile[4 * d : 4 * d + 4]
        return carry

    with jax.named_scope("weights_in"):
        lax.fori_loop(0, 8, weights_in, 0)

    owned(0, early)
    spectra = mine[...]
    for a in range(4):
        e = jnp.where(
            sub < 4,
            jnp.broadcast_to(spectra[a : a + 1], (8, LANES)),
            jnp.broadcast_to(spectra[4 + a : 5 + a], (8, LANES)),
        )
        rolled = [e] + [pltpu.roll(e, 16 * m, 1) for m in range(1, 8)]
        for q in range(8):
            copies = rolled[(0 - q) % 8]
            for t in range(1, 8):
                copies = jnp.where(lane // 16 == t, rolled[(t - q) % 8], copies)
            sv[4 * a + q // 2, q % 2] = copies

    zero = jnp.zeros((8, LANES), jnp.float32)

    def contract(i, sums):
        s_re, s_im = sv[i, 0], sv[i, 1]
        first = tuple(sums[d] + s_re * wt[i, d] for d in range(chans))
        second = tuple(sums[chans + d] + s_im * wt[i, d] for d in range(chans))
        return first + second

    sums = lax.fori_loop(0, 16, contract, (zero,) * (2 * chans), unroll=4)
    for d in range(chans):
        tx_chan[d] = sums[d] - turned(sums[chans + d])

    def to_chan(slot, k, src, dst):
        return pltpu.make_async_remote_copy(
            src_ref=src, dst_ref=dst, send_sem=csend.at[slot], recv_sem=crecv.at[slot],
            device_id={"chan": lax.rem(ch + k, chans)}, device_id_type=MESH,
        )

    for k in range(1, chans):
        to_chan(0, k, tx_chan.at[lax.rem(ch + k, chans)], rx_chan.at[chans - 1 - k]).start()
    with scope("chan_wait"):
        wait_bytes(rx_chan, crecv.at[0])
    modes_out = tx_chan[ch]
    for k in range(chans - 1):
        modes_out = modes_out + rx_chan[k]

    def everywhere(turn, tile):
        rx_modes[turn, 0] = tile
        with scope("modes_send"):
            by_core(functools.partial(spread, turn))

    def spread(turn, plan):
        rx = rx_modes.at[turn]
        chain, first, last = plan
        order = [k for k, _ in chain[:2]] + first + [k for k, _ in chain[2:]] + last
        kinds = [k for k, _ in chain]
        for k in order:
            sem = hrecv.at[turn, kinds.index(k)] if k in kinds else arecv.at[turn]
            to_slab(k, rx.at[0], rx.at[slot_of(-k)], ssend.at[2 + turn, 0], sem)

    def passed_on(turn, plan):
        rx = rx_modes.at[turn]
        by_distance = sorted(enumerate(plan[0]), key=lambda e: abs(e[1][0]))
        for n, (k, reach) in by_distance:
            held = rx.at[slot_of(-k)]
            with scope("hub_wait"):
                wait_bytes(held, hrecv.at[turn, n])
            for j in range(reach, 0, -1):
                step = j if k > 0 else -j
                to_slab(step, held, rx.at[slot_of(-k - step)], ssend.at[2 + turn, 1], arecv.at[turn])

    def all_modes(turn, plan):
        wait_bytes(rx_modes.at[turn, pl.ds(0, slabs - 1 - len(plan[0]))], arecv.at[turn])

    def rows_back(turn):
        with scope("modes_wait"):
            by_core(functools.partial(all_modes, turn))
        with scope("back_dot"):
            found = rx_modes[turn].reshape(8 * slabs, LANES)
            both = dot3((fth[...], ftl[...]), split(found))
            own_g[turn] = both[:LANES] - turned(both[LANES:])
        with scope("back_pair"):
            copy = to_mode(2 + turn, own_g.at[turn], rx_g.at[turn])
            copy.start()
            copy.wait()

    everywhere(0, modes_out * weights)
    loads[1].wait()
    by_core(functools.partial(passed_on, 0))
    rows_back(0)

    def gelu_chunk(a, carry):
        gates, biases = carry
        branch = column_synthesis(own_g.at[0], rx_g.at[0], a, rows, (tth, ttl))
        grads = []
        for b in range(4):
            c = 4 * a + b
            here = pl.ds(c * rows, rows)
            x = xv[here, :]
            v = branch[b * rows : (b + 1) * rows] + gain[c] * x + bias[c]
            v2 = v * v
            t = jnp.tanh(GELU_SLOPE * (v + GELU_CUBE * (v2 * v)))
            cdf = 0.5 * (1.0 + t)
            ov[here, :] = v * cdf
            slope = cdf + (0.5 * GELU_SLOPE) * (v * (1.0 - t * t)) * (1.0 + (3.0 * GELU_CUBE) * v2)
            grad = cv[here, :] * slope
            gv[here, :] = gain[c] * grad
            grads.append(grad)
            gate = jnp.sum(jnp.sum(grad * x, axis=0, keepdims=True), axis=1, keepdims=True)
            plain = jnp.sum(jnp.sum(grad, axis=0, keepdims=True), axis=1, keepdims=True)
            spot = iota((1, LANES), 1) == c
            gates = jnp.where(spot, gate, gates)
            biases = jnp.where(spot, plain, biases)
        tx_cols[1, pl.ds(a * rows, rows), :] = column_forward(a, jnp.concatenate(grads, axis=0))
        return gates, biases

    empty = jnp.zeros((1, LANES), jnp.float32)
    with scope("gelu"):
        gates, biases = lax.fori_loop(0, 4, gelu_chunk, (empty, empty), unroll=True)
    rows_forward(1)

    red_pair[0] = jnp.concatenate([gates, biases], axis=0)
    with scope("pair_sums"):
        copy = to_mode(4, red_pair.at[0], red_pair.at[1])
        copy.start()
        copy.wait()
        red_pair[2] = red_pair[0] + red_pair[1]
        for j in range(1, 4):
            pltpu.make_async_remote_copy(
                src_ref=red_pair.at[2], dst_ref=red_near.at[j - 1], send_sem=rsend.at[0], recv_sem=rrecv.at[0],
                device_id={"slab": me ^ j}, device_id_type=MESH,
            ).start()

    by_core(functools.partial(hub_sums, 1))
    near_sums()
    by_core(functools.partial(owned, 1))
    g_chan[ch] = mine[...] * weights
    for k in range(1, chans):
        to_chan(1, k, g_chan.at[ch], g_chan.at[ch]).start()
    with scope("chan_wait_two"):
        wait_bytes(g_chan.at[pl.ds(0, chans - 1)], crecv.at[1])
    g_all = [g_chan[d] for d in range(chans)]
    g_turned = [turned(g) for g in g_all]

    def contract_back(i):
        first, second = zero, zero
        for d in range(chans):
            w = wt[i, d]
            first = first + w * g_all[d]
            second = second + w * g_turned[d]
        v = jnp.where(real_part, first + pltpu.roll(first, 16, 1), second + pltpu.roll(second, 16, 1))
        v = v + pltpu.roll(v, 32, 1)
        return v + pltpu.roll(v, 64, 1)

    back = zero
    for a in range(4):
        m = contract_back(4 * a)
        for b in range(1, 4):
            m = jnp.where(lane // 32 == b, contract_back(4 * a + b), m)
        for x in range(2):
            row = jnp.sum(m[4 * x : 4 * x + 4], axis=0, keepdims=True)
            back = jnp.where(sub == 4 * x + a, jnp.broadcast_to(row, (8, LANES)), back)
    everywhere(1, back)

    def weights_out(pair, carry):
        tiles = []
        for t in range(4):
            i = 2 * pair + t // 2
            if t % 2 == 0:
                s_re, s_im = sv[i, 0], sv[i, 1]
                made = [s_re * g_all[d] + s_im * g_turned[d] for d in range(chans)]
            parts = [made[d][4 * (t % 2) : 4 * (t % 2) + 4] for d in range(chans)]
            tile = jnp.concatenate(parts, axis=0)
            tiles.append(jnp.where(ch * 16 + i < reads, tile, 0.0))
        for b in range(4):
            low = jnp.zeros((16, LANES), jnp.float32)
            for t in range(4):
                shift = 32 * ((t - b) % 4)
                moved = pltpu.roll(tiles[t], shift, 1) if shift else tiles[t]
                low = jnp.where(lane16 // 32 == t, moved, low)
            zs[pl.ds(b, 16, stride=4), :] = low
        back_rows = zs[...].T
        for t in range(4):
            for p in range(2):
                at = 32 * t + 16 * p
                sgv[2 * pair + t // 2, pl.ds(2 * p + t % 2, 16, stride=4), :] = back_rows[at : at + 16]
        return carry

    with scope("weights_out"):
        lax.fori_loop(0, 8, weights_out, 0)
    by_core(functools.partial(passed_on, 1))
    rows_back(1)
    last_own[...] = own_g[1]
    last_rx[...] = rx_g[1]
    wait_bytes(red_far, rrecv.at[1])
    total = red_pair[3]
    for m in range(slabs // 4 - 1):
        total = total + red_far[m]
    gate_ref[...] = total[0:1, :16]
    bgrad_ref[...] = total[1:2, :16]
    def rows_sent(turn, plan):
        chain, first, last = plan
        wait_bytes(rx_far.at[turn, pl.ds(0, len(first) + len(last))], ssend.at[turn, 0])
        wait_bytes(tx_rows.at[turn, pl.ds(0, sum(reach for _, reach in chain))], ssend.at[turn, 1])
        wait_bytes(tx_far.at[turn, pl.ds(0, len(chain))], ssend.at[turn, 2])

    def modes_sent(turn, plan):
        passed = sum(reach for _, reach in plan[0])
        wait_bytes(rx_modes.at[turn, pl.ds(0, slabs - 1 - passed)], ssend.at[2 + turn, 0])
        wait_bytes(rx_modes.at[turn, pl.ds(0, passed)], ssend.at[2 + turn, 1])

    rows_sent(0, early)
    by_core(functools.partial(rows_sent, 1))
    for turn in range(2):
        by_core(functools.partial(modes_sent, turn))
        wait_bytes(rx_chan, csend.at[turn])
    wait_bytes(red_near, rsend.at[0])
    wait_bytes(red_far, rsend.at[1])


def column_synthesis(own, theirs, a, rows, tables):
    here = pl.ds(a * rows, rows)
    g = jnp.concatenate([own[here, :], theirs[here, :]], axis=1)
    block = (iota(g.shape, 1) & (LANES - 1)) // 32
    spread = jnp.concatenate([jnp.where(block == b, g, 0.0) for b in range(4)], axis=0)
    return dot3(split(spread), (tables[0][...], tables[1][...]))


def finish(
    rows, ov, gv, sgv, gate, bgrad, own, theirs, tth, ttl,
    out_hbm, fgrad_hbm, sgrad_hbm, gate_hbm, bgrad_hbm,
    fv, sem, fsem,
):
    pairs = ((ov, out_hbm), (sgv, sgrad_hbm), (gate, gate_hbm), (bgrad, bgrad_hbm))
    copies = [pltpu.make_async_copy(a, b, sem.at[n]) for n, (a, b) in enumerate(pairs)]
    for copy in copies:
        copy.start()
    chunk = 4 * rows
    for a in range(4):
        here = pl.ds(a * chunk, chunk)
        fv[here, :] = column_synthesis(own, theirs, a, rows, (tth, ttl)) + gv[here, :]
        copies.append(pltpu.make_async_copy(fv.at[here, :], fgrad_hbm.at[here, :], fsem.at[a]))
        copies[-1].start()
    for copy in copies:
        copy.wait()


def local(source_field, cotangent, spectral_weight, skip_gain, channel_bias, mode_limit, width_limit):
    channels, rows, cols = source_field.shape
    slabs, chans, modes = lax.axis_size("slab"), lax.axis_size("chan"), lax.axis_size("mode")
    outs = spectral_weight.shape[1]
    assert (channels, rows, modes, outs) == (16, 32, 2, 16 * chans)
    assert spectral_weight.shape[2:] == (16, 2, 2)
    flat = (channels * rows, cols)
    w = spectral_weight.transpose(0, 2, 3, 4, 1).reshape(channels, 64, outs)
    limits = mode_limit.T
    f32, bf16 = jnp.float32, jnp.bfloat16
    vmem, sems = pltpu.VMEM, pltpu.SemaphoreType.DMA
    hubs = slabs // 8 - 1
    plans = early_plan(slabs), *main_plans(slabs)
    chains = max(len(p[0]) for p in plans)
    arrivals = max(sum(map(len, p)) for p in plans)
    reach = max(r for p in plans for _, r in p[0])
    assert all(sum(r for _, r in p[0]) + sum(map(len, p)) == slabs - 1 for p in plans)
    hbm_spec = pl.BlockSpec(memory_space=pltpu.HBM)
    vmem_spec = pl.BlockSpec(memory_space=pltpu.VMEM)
    square = (LANES, LANES)
    held = (
        (flat, f32), (flat, f32), (w.shape, f32), ((1, channels), f32), ((1, channels), f32),
        (square, f32), (square, f32), ((2 * LANES, cols), bf16), ((2 * LANES, cols), bf16),
    )
    found = pl.pallas_call(
        functools.partial(kernel, (slabs, chans, modes, rows, cols)),
        out_shape=tuple(jax.ShapeDtypeStruct(*h) for h in held),
        in_specs=[hbm_spec] * 7,
        out_specs=[vmem_spec] * len(held),
        scratch_shapes=[
            vmem(flat, f32), vmem(flat, f32), vmem(w.shape, f32),
            pltpu.SMEM(skip_gain.shape, f32), pltpu.SMEM(channel_bias.shape, f32),
            pltpu.SMEM(limits.shape, jnp.int32), pltpu.SMEM(width_limit.shape, jnp.int32),
            vmem((cols, 2 * LANES), bf16), vmem((cols, 2 * LANES), bf16),
            vmem((8 * slabs, 2 * LANES), bf16), vmem((8 * slabs, 2 * LANES), bf16),
            vmem((2 * LANES, 8 * slabs), bf16), vmem((2 * LANES, 8 * slabs), bf16),
            vmem((channels, chans, 8, LANES), f32), vmem((outs, LANES), f32),
            vmem((channels, 2, 8, LANES), f32),
            vmem(square, f32), vmem((2, *square), f32), vmem((2, *square), f32),
            vmem((2, slabs, 8, LANES), f32), vmem((2, chains, reach, 8, LANES), f32),
            vmem((2, chains, 8, LANES), f32), vmem((2, arrivals, 8, LANES), f32),
            vmem((chans, 8, LANES), f32), vmem((chans - 1, 8, LANES), f32),
            vmem((2, slabs, 8, LANES), f32), vmem((8, LANES), f32),
            vmem((2, *square), f32), vmem((2, *square), f32),
            vmem((chans, 8, LANES), f32), vmem((4, 2, LANES), f32),
            vmem((3, 2, LANES), f32), vmem((slabs // 4 - 1, 2, LANES), f32),
            sems((7,)), sems((5,)), sems((5,)), sems((4, 3)), sems((2, chains)), sems((2,)),
            sems((2, chains)), sems((2,)), sems((2,)), sems((2,)), sems((2,)), sems((2,)),
        ],
        compiler_params=pltpu.CompilerParams(collective_id=0, has_side_effects=True, vmem_limit_bytes=40 << 20),
        name="fno_layer",
    )(
        *(
            pltpu.with_memory_space_constraint(a, pltpu.HBM)
            for a in (
                source_field.reshape(flat), cotangent.reshape(flat), w, skip_gain, channel_bias, limits, width_limit,
            )
        )
    )
    out, fgrad, sgrad, gate, bgrad = pl.pallas_call(
        functools.partial(finish, rows),
        out_shape=tuple(jax.ShapeDtypeStruct(*h) for h in held[:5]),
        in_specs=[vmem_spec] * len(held),
        out_specs=[hbm_spec] * 5,
        scratch_shapes=[vmem(flat, f32), pltpu.SemaphoreType.DMA((4,)), pltpu.SemaphoreType.DMA((4,))],
        compiler_params=pltpu.CompilerParams(vmem_limit_bytes=24 << 20),
        name="fno_finish",
    )(*found)
    sgrad = sgrad.reshape(channels, 16, 2, 2, outs).transpose(0, 4, 1, 2, 3)
    return (
        out.reshape(source_field.shape), fgrad.reshape(source_field.shape), sgrad,
        gate.reshape(channels), bgrad.reshape(channels),
    )


def solution(mesh):
    field = P(("member", "chan"), "slab", "mode")
    weight = P(("member", "chan"), None, "mode", None, "slab")
    channel = P(("member", "chan"))
    return jax.shard_map(
        local,
        mesh=mesh,
        in_specs=(field, field, weight, channel, channel, P("member", None), P("member")),
        out_specs=(field, field, weight, channel, channel),
        check_vma=False,
    )
```

```python
import functools
import math

import jax
import jax.numpy as jnp
from jax import lax
from jax.experimental import pallas as pl
from jax.experimental.pallas import tpu as pltpu
from jax.sharding import PartitionSpec as P

MESH = pl.DeviceIdType.MESH
LANES = 128
GELU_SLOPE = math.sqrt(2.0 / math.pi)
GELU_CUBE = 0.044715


def slab_offsets(slabs):
    hubs = slabs // 8 - 1
    far = [4 * m for m in range(1, hubs + 1)]
    found = [0, slabs // 2] + far + [-k for k in far]
    for sign in (1, -1):
        for j in range(1, 4):
            found += [sign * (j + 4 * m) for m in range(hubs + 1)]
    return found


def both_ways(ks):
    return [sign * k for k in ks for sign in (1, -1)]


def early_plan(slabs):
    top = slabs // 4
    hubs = [(top, slabs // 2 - top), (-top, slabs // 2 - top - 1), (4, top - 5), (-4, top - 5)]
    return hubs, [], both_ways((3, 2, 1))


def main_plans(slabs):
    half = slabs // 2
    hubs = [(k, half // 2 - 4 if abs(k) > 4 else 3) for k in both_ways((half // 2, 4))]
    first = [half] + both_ways(range(half - 1, half - 4, -1))
    many = [(k, 3) for k in both_ways(range(half - 4, 0, -4))]
    return (hubs, first, both_ways((3, 2, 1))), (many, [half], both_ways((3, 2, 1)))


def offset_of(slot, slabs):
    hubs = slabs // 8 - 1
    first = 2 + 2 * hubs
    near = jnp.where(slot < 2 + hubs, 4 * (slot - 1), -4 * (slot - 1 - hubs))
    group, m = (slot - first) // (hubs + 1), (slot - first) % (hubs + 1)
    behind = jnp.where(group < 3, 1 + group + 4 * m, -(group - 2) - 4 * m)
    found = jnp.where(slot < first, near, behind)
    return jnp.where(slot == 0, 0, jnp.where(slot == 1, slabs // 2, found))


def split(x):
    high = x.astype(jnp.bfloat16)
    low = (x - high.astype(jnp.float32)).astype(jnp.bfloat16)
    return high, low


def dot3(a, b):
    (ah, al), (bh, bl) = a, b
    dot = functools.partial(jnp.dot, preferred_element_type=jnp.float32)
    return dot(ah, bh) + (dot(ah, bl) + dot(al, bh))


def sine(turns, extent):
    half, quarter = extent // 2, extent // 4
    t = ((turns + half) & (extent - 1)) - half
    t = jnp.where(t > quarter, half - t, jnp.where(t < -quarter, -half - t, t))
    v = t.astype(jnp.float32) * (2.0 * math.pi / extent)
    s = v * v
    poly = -2.5052108e-8
    for c in (2.7557319e-6, -1.9841270e-4, 8.3333333e-3, -1.6666667e-1, 1.0):
        poly = poly * s + c
    return poly * v


def iota(shape, dim):
    return lax.broadcasted_iota(jnp.int32, shape, dim)


def kernel(
    dims,
    x_hbm, cot_hbm, w_hbm, gain_hbm, bias_hbm, limit_hbm, width_hbm,
    ov, gv, sgv, gate_ref, bgrad_ref, last_own, last_rx, tth, ttl,
    xv, cv, wv, gain, bias, limit, width, tch, tcl, fh, fl, fth, ftl,
    wt, zs, sv,
    own_cols, tx_cols, rx_cols, tx_rows, rx_near, tx_far, rx_far, tx_chan, rx_chan, rx_modes, mine,
    own_g, rx_g, g_chan, red_pair, red_near, red_far,
    lsem, msend, mrecv, ssend, nrecv, frecv, hrecv, arecv, csend, crecv, rsend, rrecv,
):
    slabs, chans, modes, rows, cols = dims
    chunk = 4 * rows
    me, ch, mo = lax.axis_index("slab"), lax.axis_index("chan"), lax.axis_index("mode")
    other = 1 - mo
    all_rows, all_cols = slabs * rows, modes * cols
    kx_count = 2 * slabs

    scope = jax.named_scope
    barrier = pltpu.get_barrier_semaphore()

    hubs = slabs // 8 - 1
    offsets = slab_offsets(slabs)
    partners = sorted((k for k in offsets if 0 < abs(k) <= slabs // 4), key=lambda k: -abs(k))
    early, mains = early_plan(slabs), main_plans(slabs)

    def by_core(f):
        for core, plan in enumerate(mains):
            pl.when(mo == core)(functools.partial(f, plan))

    def slot_of(k):
        k %= slabs
        return offsets.index(k - slabs if k > slabs // 2 else k)

    def slab_at(k):
        return {"slab": (me + k + slabs) & (slabs - 1)}

    with scope("greet"):
        for k in partners:
            pl.semaphore_signal(barrier, inc=1, device_id=slab_at(k), device_id_type=MESH)
    for k in range(1, chans):
        pl.semaphore_signal(barrier, inc=1, device_id={"chan": lax.rem(ch + k, chans)}, device_id_type=MESH)
    pl.semaphore_signal(barrier, inc=1, device_id={"mode": other}, device_id_type=MESH)

    pairs = (
        (x_hbm, xv), (cot_hbm, cv), (w_hbm, wv), (limit_hbm, limit), (width_hbm, width),
        (gain_hbm, gain), (bias_hbm, bias),
    )
    loads = [pltpu.make_async_copy(a, b, lsem.at[n]) for n, (a, b) in enumerate(pairs)]
    for load in loads:
        load.start()
    def to_mode(slot, src, dst):
        return pltpu.make_async_remote_copy(
            src_ref=src, dst_ref=dst, send_sem=msend.at[slot], recv_sem=mrecv.at[slot],
            device_id={"mode": other}, device_id_type=MESH,
        )

    def to_slab(k, src, dst, send_sem, recv_sem):
        pltpu.make_async_remote_copy(
            src_ref=src, dst_ref=dst, send_sem=send_sem, recv_sem=recv_sem,
            device_id=slab_at(k), device_id_type=MESH,
        ).start()

    def wait_bytes(ref, sem):
        pltpu.make_async_copy(ref, ref, sem).wait()

    lane = iota((8, LANES), 1)
    real_part = lane % 32 < 16

    def turned(v):
        re = iota(v.shape, 1) & 31 < 16
        return jnp.where(re, pltpu.roll(v, LANES - 16, 1), -pltpu.roll(v, 16, 1))

    def column_angles(n, w):
        holder = jnp.where(n < LANES, mo, other)
        freq = holder * 16 + (n & 15)
        cell = mo * cols + w
        return freq * cell + jnp.where(n & 31 < 16, all_cols // 4, all_cols // 2)

    with scope("column_table"):
        shape = (cols, 2 * LANES)
        tch[...], tcl[...] = split(sine(column_angles(iota(shape, 1), iota(shape, 0)), all_cols))

    def row_angles(k, n):
        kx = 2 * ((me + offset_of(k >> 3, slabs) + slabs) & (slabs - 1)) + ((k >> 2) & 1)
        kx = jnp.where(kx < kx_count // 2, kx, kx + all_rows - kx_count)
        half = LANES
        cell = me * rows + (n & (rows - 1))
        angle = kx * cell + jnp.where(n < half, all_rows // 4, 0)
        same = (k & 3) == ((n & (half - 1)) // rows)
        return jnp.where(same, sine(angle, all_rows), 0.0)

    def column_forward(a, values):
        d = dot3(split(values), (tch[...], tcl[...]))
        block = (iota((rows, 2 * LANES), 1) % LANES) // 32
        packed = d[:rows]
        for b in range(1, 4):
            packed = jnp.where(block == b, d[b * rows : (b + 1) * rows], packed)
        own_cols[pl.ds(a * rows, rows), :] = packed[:, :LANES]
        return packed[:, LANES:]

    with scope("row_table"):
        shape = (8 * slabs, 2 * LANES)
        fh[...], fl[...] = split(row_angles(iota(shape, 0), iota(shape, 1)))

    with scope("load_wait"):
        loads[0].wait()

    def first_chunk(a, carry):
        values = xv[pl.ds(a * chunk, chunk), :]
        tx_cols[0, pl.ds(a * rows, rows), :] = column_forward(a, values)
        return carry

    with scope("first_columns"):
        lax.fori_loop(0, 4, first_chunk, 0, unroll=True)
    with scope("barrier_wait"):
        pl.semaphore_wait(barrier, len(partners) + chans - 1 + 1)

    def rows_forward(turn):
        copy = to_mode(turn, tx_cols.at[turn], rx_cols.at[turn])
        copy.start()
        with scope("columns_pair"):
            copy.wait()
        with scope("rows_dot"):
            lined = own_cols[...] + rx_cols[turn]
            both = jnp.concatenate([lined, turned(lined)], axis=0)
            partial = dot3((fh[...], fl[...]), split(both))
            tx_rows[turn] = partial.reshape(slabs, 8, LANES)
        def send(plan):
            chain, first, last = plan

            def near(n):
                k, reach = chain[n]
                for j in range(reach, 0, -1):
                    step = j if k > 0 else -j
                    to_slab(
                        step, tx_rows.at[turn, slot_of(k + step)], rx_near.at[turn, n, j - 1],
                        ssend.at[turn, 1], nrecv.at[turn, n],
                    )

            def direct(ks, at):
                for n, k in enumerate(ks):
                    to_slab(k, tx_rows.at[turn, slot_of(k)], rx_far.at[turn, at + n], ssend.at[turn, 0], frecv.at[turn])

            near(0)
            near(1)
            direct(first, len(chain))
            for n in range(2, len(chain)):
                near(n)
            direct(last, len(chain) + len(first))

        with scope("rows_send"):
            by_core(send) if turn else send(early)

    def hub_sums(turn, plan):
        for n, (k, reach) in enumerate(plan[0]):
            with scope("near_wait"):
                wait_bytes(rx_near.at[turn, n, pl.ds(0, reach)], nrecv.at[turn, n])
            total = tx_rows[turn, slot_of(k)]
            for j in range(reach):
                total = total + rx_near[turn, n, j]
            tx_far[turn, n] = total
            to_slab(k, tx_far.at[turn, n], rx_far.at[turn, n], ssend.at[turn, 2], frecv.at[turn])
    def near_sums():
        with scope("sums_near"):
            wait_bytes(red_near, rrecv.at[0])
            total = red_pair[2]
            for j in range(3):
                total = total + red_near[j]
            red_pair[3] = total
            for m in range(1, slabs // 4):
                to_slab(4 * m, red_pair.at[3], red_far.at[m - 1], rsend.at[1], rrecv.at[1])

    def owned(turn, plan):
        count = sum(map(len, plan))
        with scope("rows_wait"):
            wait_bytes(rx_far.at[turn, pl.ds(0, count)], frecv.at[turn])
        total = tx_rows[turn, 0]
        for n in range(count):
            total = total + rx_far[turn, n]
        mine[...] = total

    rows_forward(0)
    hub_sums(0, early)

    with scope("back_tables"):
        shape = (2 * LANES, cols)
        tth[...], ttl[...] = split(sine(column_angles(iota(shape, 0), iota(shape, 1)), all_cols))
        shape = (2 * LANES, 8 * slabs)
        fth[...], ftl[...] = split(row_angles(iota(shape, 1), iota(shape, 0)))

    for load in loads[3:]:
        load.wait()
    sub = iota((8, LANES), 0)
    keep_col = jnp.zeros((8, LANES), jnp.int32)
    keep_row = jnp.zeros((8, LANES), jnp.int32)
    for c in range(16):
        here = (sub % 4 == c // 4) & (lane // 32 == c % 4)
        keep_col = jnp.where(here, limit[0, ch * 16 + c], keep_col)
        keep_row = jnp.where(here, limit[1, ch * 16 + c], keep_row)
    col_freq = mo * 16 + lane % 16
    row_freq = me * 2 + sub // 4
    kept = (col_freq < keep_col) & ((row_freq < keep_row) | (kx_count - row_freq < keep_row))
    scale = jnp.where(col_freq == 0, 1.0, 2.0) / (all_rows * all_cols)
    weights = jnp.where(kept, scale, 0.0)

    sub16 = iota((16, LANES), 0)
    lane16 = iota((16, LANES), 1)
    reads = jnp.zeros((16, LANES), jnp.int32)
    for o in range(16 * chans):
        reads = jnp.where((sub16 == o // 4) & (lane16 // 32 == o % 4), width[o], reads)

    loads[2].wait()

    def weights_in(pair, carry):
        parts = []
        for t in range(4):
            for p in range(2):
                parts.append(wv[2 * pair + t // 2, pl.ds(2 * p + t % 2, 16, stride=4), :])
        zs[...] = jnp.concatenate(parts, axis=0).T
        by_low = [zs[pl.ds(b, 16, stride=4), :] for b in range(4)]
        for t in range(4):
            i = 2 * pair + t // 2
            tile = jnp.zeros((16, LANES), jnp.float32)
            for b in range(4):
                shift = 32 * ((b - t) % 4)
                moved = pltpu.roll(by_low[b], shift, 1) if shift else by_low[b]
                tile = jnp.where(lane16 // 32 == b, moved, tile)
            tile = jnp.where(ch * 16 + i < reads, tile, 0.0)
            for d in range(chans):
                wt[i, d, pl.ds(4 * (t % 2), 4), :] = tile[4 * d : 4 * d + 4]
        return carry

    with jax.named_scope("weights_in"):
        lax.fori_loop(0, 8, weights_in, 0)

    owned(0, early)
    spectra = mine[...]
    for a in range(4):
        e = jnp.where(
            sub < 4,
            jnp.broadcast_to(spectra[a : a + 1], (8, LANES)),
            jnp.broadcast_to(spectra[4 + a : 5 + a], (8, LANES)),
        )
        rolled = [e] + [pltpu.roll(e, 16 * m, 1) for m in range(1, 8)]
        for q in range(8):
            copies = rolled[(0 - q) % 8]
            for t in range(1, 8):
                copies = jnp.where(lane // 16 == t, rolled[(t - q) % 8], copies)
            sv[4 * a + q // 2, q % 2] = copies

    zero = jnp.zeros((8, LANES), jnp.float32)

    def contract(i, sums):
        s_re, s_im = sv[i, 0], sv[i, 1]
        first = tuple(sums[d] + s_re * wt[i, d] for d in range(chans))
        second = tuple(sums[chans + d] + s_im * wt[i, d] for d in range(chans))
        return first + second

    sums = lax.fori_loop(0, 16, contract, (zero,) * (2 * chans), unroll=4)
    for d in range(chans):
        tx_chan[d] = sums[d] - turned(sums[chans + d])

    def to_chan(slot, k, src, dst):
        return pltpu.make_async_remote_copy(
            src_ref=src, dst_ref=dst, send_sem=csend.at[slot], recv_sem=crecv.at[slot],
            device_id={"chan": lax.rem(ch + k, chans)}, device_id_type=MESH,
        )

    for k in range(1, chans):
        to_chan(0, k, tx_chan.at[lax.rem(ch + k, chans)], rx_chan.at[chans - 1 - k]).start()
    with scope("chan_wait"):
        wait_bytes(rx_chan, crecv.at[0])
    modes_out = tx_chan[ch]
    for k in range(chans - 1):
        modes_out = modes_out + rx_chan[k]

    def everywhere(turn, tile):
        rx_modes[turn, 0] = tile
        with scope("modes_send"):
            by_core(functools.partial(spread, turn))

    def spread(turn, plan):
        rx = rx_modes.at[turn]
        chain, first, last = plan
        order = [k for k, _ in chain[:2]] + first + [k for k, _ in chain[2:]] + last
        kinds = [k for k, _ in chain]
        for k in order:
            sem = hrecv.at[turn, kinds.index(k)] if k in kinds else arecv.at[turn]
            to_slab(k, rx.at[0], rx.at[slot_of(-k)], ssend.at[2 + turn, 0], sem)

    def passed_on(turn, plan):
        rx = rx_modes.at[turn]
        by_distance = sorted(enumerate(plan[0]), key=lambda e: abs(e[1][0]))
        for n, (k, reach) in by_distance:
            held = rx.at[slot_of(-k)]
            with scope("hub_wait"):
                wait_bytes(held, hrecv.at[turn, n])
            for j in range(reach, 0, -1):
                step = j if k > 0 else -j
                to_slab(step, held, rx.at[slot_of(-k - step)], ssend.at[2 + turn, 1], arecv.at[turn])

    def all_modes(turn, plan):
        wait_bytes(rx_modes.at[turn, pl.ds(0, slabs - 1 - len(plan[0]))], arecv.at[turn])

    def rows_back(turn):
        with scope("modes_wait"):
            by_core(functools.partial(all_modes, turn))
        with scope("back_dot"):
            found = rx_modes[turn].reshape(8 * slabs, LANES)
            both = dot3((fth[...], ftl[...]), split(found))
            own_g[turn] = both[:LANES] - turned(both[LANES:])
        with scope("back_pair"):
            copy = to_mode(2 + turn, own_g.at[turn], rx_g.at[turn])
            copy.start()
            copy.wait()

    everywhere(0, modes_out * weights)
    loads[1].wait()
    by_core(functools.partial(passed_on, 0))
    rows_back(0)

    def gelu_chunk(a, carry):
        gates, biases = carry
        branch = column_synthesis(own_g.at[0], rx_g.at[0], a, rows, (tth, ttl))
        grads = []
        for b in range(4):
            c = 4 * a + b
            here = pl.ds(c * rows, rows)
            x = xv[here, :]
            v = branch[b * rows : (b + 1) * rows] + gain[c] * x + bias[c]
            v2 = v * v
            t = jnp.tanh(GELU_SLOPE * (v + GELU_CUBE * (v2 * v)))
            cdf = 0.5 * (1.0 + t)
            ov[here, :] = v * cdf
            slope = cdf + (0.5 * GELU_SLOPE) * (v * (1.0 - t * t)) * (1.0 + (3.0 * GELU_CUBE) * v2)
            grad = cv[here, :] * slope
            gv[here, :] = gain[c] * grad
            grads.append(grad)
            gate = jnp.sum(jnp.sum(grad * x, axis=0, keepdims=True), axis=1, keepdims=True)
            plain = jnp.sum(jnp.sum(grad, axis=0, keepdims=True), axis=1, keepdims=True)
            spot = iota((1, LANES), 1) == c
            gates = jnp.where(spot, gate, gates)
            biases = jnp.where(spot, plain, biases)
        tx_cols[1, pl.ds(a * rows, rows), :] = column_forward(a, jnp.concatenate(grads, axis=0))
        return gates, biases

    empty = jnp.zeros((1, LANES), jnp.float32)
    with scope("gelu"):
        gates, biases = lax.fori_loop(0, 4, gelu_chunk, (empty, empty), unroll=True)
    rows_forward(1)

    red_pair[0] = jnp.concatenate([gates, biases], axis=0)
    with scope("pair_sums"):
        copy = to_mode(4, red_pair.at[0], red_pair.at[1])
        copy.start()
        copy.wait()
        red_pair[2] = red_pair[0] + red_pair[1]
        for j in range(1, 4):
            pltpu.make_async_remote_copy(
                src_ref=red_pair.at[2], dst_ref=red_near.at[j - 1], send_sem=rsend.at[0], recv_sem=rrecv.at[0],
                device_id={"slab": me ^ j}, device_id_type=MESH,
            ).start()

    by_core(functools.partial(hub_sums, 1))
    near_sums()
    by_core(functools.partial(owned, 1))
    g_chan[ch] = mine[...] * weights
    for k in range(1, chans):
        to_chan(1, k, g_chan.at[ch], g_chan.at[ch]).start()
    with scope("chan_wait_two"):
        wait_bytes(g_chan.at[pl.ds(0, chans - 1)], crecv.at[1])
    g_all = [g_chan[d] for d in range(chans)]
    g_turned = [turned(g) for g in g_all]

    def contract_back(i):
        first, second = zero, zero
        for d in range(chans):
            w = wt[i, d]
            first = first + w * g_all[d]
            second = second + w * g_turned[d]
        v = jnp.where(real_part, first + pltpu.roll(first, 16, 1), second + pltpu.roll(second, 16, 1))
        v = v + pltpu.roll(v, 32, 1)
        return v + pltpu.roll(v, 64, 1)

    back = zero
    for a in range(4):
        m = contract_back(4 * a)
        for b in range(1, 4):
            m = jnp.where(lane // 32 == b, contract_back(4 * a + b), m)
        for x in range(2):
            row = jnp.sum(m[4 * x : 4 * x + 4], axis=0, keepdims=True)
            back = jnp.where(sub == 4 * x + a, jnp.broadcast_to(row, (8, LANES)), back)
    everywhere(1, back)

    def weights_out(pair, carry):
        tiles = []
        for t in range(4):
            i = 2 * pair + t // 2
            if t % 2 == 0:
                s_re, s_im = sv[i, 0], sv[i, 1]
                made = [s_re * g_all[d] + s_im * g_turned[d] for d in range(chans)]
            parts = [made[d][4 * (t % 2) : 4 * (t % 2) + 4] for d in range(chans)]
            tile = jnp.concatenate(parts, axis=0)
            tiles.append(jnp.where(ch * 16 + i < reads, tile, 0.0))
        for b in range(4):
            low = jnp.zeros((16, LANES), jnp.float32)
            for t in range(4):
                shift = 32 * ((t - b) % 4)
                moved = pltpu.roll(tiles[t], shift, 1) if shift else tiles[t]
                low = jnp.where(lane16 // 32 == t, moved, low)
            zs[pl.ds(b, 16, stride=4), :] = low
        back_rows = zs[...].T
        for t in range(4):
            for p in range(2):
                at = 32 * t + 16 * p
                sgv[2 * pair + t // 2, pl.ds(2 * p + t % 2, 16, stride=4), :] = back_rows[at : at + 16]
        return carry

    with scope("weights_out"):
        lax.fori_loop(0, 8, weights_out, 0)
    by_core(functools.partial(passed_on, 1))

    wait_bytes(red_far, rrecv.at[1])
    total = red_pair[3]
    for m in range(slabs // 4 - 1):
        total = total + red_far[m]
    gate_ref[...] = total[0:1, :16]
    bgrad_ref[...] = total[1:2, :16]
    def rows_sent(turn, plan):
        chain, first, last = plan
        wait_bytes(rx_far.at[turn, pl.ds(0, len(first) + len(last))], ssend.at[turn, 0])
        wait_bytes(tx_rows.at[turn, pl.ds(0, sum(reach for _, reach in chain))], ssend.at[turn, 1])
        wait_bytes(tx_far.at[turn, pl.ds(0, len(chain))], ssend.at[turn, 2])

    def modes_sent(turn, plan):
        passed = sum(reach for _, reach in plan[0])
        wait_bytes(rx_modes.at[turn, pl.ds(0, slabs - 1 - passed)], ssend.at[2 + turn, 0])
        wait_bytes(rx_modes.at[turn, pl.ds(0, passed)], ssend.at[2 + turn, 1])

    rows_sent(0, early)
    by_core(functools.partial(rows_sent, 1))
    by_core(functools.partial(modes_sent, 0))
    for turn in range(2):
        wait_bytes(rx_chan, csend.at[turn])
    wait_bytes(red_near, rsend.at[0])
    wait_bytes(red_far, rsend.at[1])

    rows_back(1)
    last_own[...] = own_g[1]
    last_rx[...] = rx_g[1]
    by_core(functools.partial(modes_sent, 1))


def column_synthesis(own, theirs, a, rows, tables):
    here = pl.ds(a * rows, rows)
    g = jnp.concatenate([own[here, :], theirs[here, :]], axis=1)
    block = (iota(g.shape, 1) & (LANES - 1)) // 32
    spread = jnp.concatenate([jnp.where(block == b, g, 0.0) for b in range(4)], axis=0)
    return dot3(split(spread), (tables[0][...], tables[1][...]))


def finish(
    rows, ov, gv, sgv, gate, bgrad, own, theirs, tth, ttl,
    out_hbm, fgrad_hbm, sgrad_hbm, gate_hbm, bgrad_hbm,
    fv, sem, fsem,
):
    pairs = ((ov, out_hbm), (sgv, sgrad_hbm), (gate, gate_hbm), (bgrad, bgrad_hbm))
    copies = [pltpu.make_async_copy(a, b, sem.at[n]) for n, (a, b) in enumerate(pairs)]
    for copy in copies:
        copy.start()
    chunk = 4 * rows
    for a in range(4):
        here = pl.ds(a * chunk, chunk)
        fv[here, :] = column_synthesis(own, theirs, a, rows, (tth, ttl)) + gv[here, :]
        copies.append(pltpu.make_async_copy(fv.at[here, :], fgrad_hbm.at[here, :], fsem.at[a]))
        copies[-1].start()
    for copy in copies:
        copy.wait()


def local(source_field, cotangent, spectral_weight, skip_gain, channel_bias, mode_limit, width_limit):
    channels, rows, cols = source_field.shape
    slabs, chans, modes = lax.axis_size("slab"), lax.axis_size("chan"), lax.axis_size("mode")
    outs = spectral_weight.shape[1]
    assert (channels, rows, modes, outs) == (16, 32, 2, 16 * chans)
    assert spectral_weight.shape[2:] == (16, 2, 2)
    flat = (channels * rows, cols)
    w = spectral_weight.transpose(0, 2, 3, 4, 1).reshape(channels, 64, outs)
    limits = mode_limit.T
    f32, bf16 = jnp.float32, jnp.bfloat16
    vmem, sems = pltpu.VMEM, pltpu.SemaphoreType.DMA
    hubs = slabs // 8 - 1
    plans = early_plan(slabs), *main_plans(slabs)
    chains = max(len(p[0]) for p in plans)
    arrivals = max(sum(map(len, p)) for p in plans)
    reach = max(r for p in plans for _, r in p[0])
    assert all(sum(r for _, r in p[0]) + sum(map(len, p)) == slabs - 1 for p in plans)
    hbm_spec = pl.BlockSpec(memory_space=pltpu.HBM)
    vmem_spec = pl.BlockSpec(memory_space=pltpu.VMEM)
    square = (LANES, LANES)
    held = (
        (flat, f32), (flat, f32), (w.shape, f32), ((1, channels), f32), ((1, channels), f32),
        (square, f32), (square, f32), ((2 * LANES, cols), bf16), ((2 * LANES, cols), bf16),
    )
    found = pl.pallas_call(
        functools.partial(kernel, (slabs, chans, modes, rows, cols)),
        out_shape=tuple(jax.ShapeDtypeStruct(*h) for h in held),
        in_specs=[hbm_spec] * 7,
        out_specs=[vmem_spec] * len(held),
        scratch_shapes=[
            vmem(flat, f32), vmem(flat, f32), vmem(w.shape, f32),
            pltpu.SMEM(skip_gain.shape, f32), pltpu.SMEM(channel_bias.shape, f32),
            pltpu.SMEM(limits.shape, jnp.int32), pltpu.SMEM(width_limit.shape, jnp.int32),
            vmem((cols, 2 * LANES), bf16), vmem((cols, 2 * LANES), bf16),
            vmem((8 * slabs, 2 * LANES), bf16), vmem((8 * slabs, 2 * LANES), bf16),
            vmem((2 * LANES, 8 * slabs), bf16), vmem((2 * LANES, 8 * slabs), bf16),
            vmem((channels, chans, 8, LANES), f32), vmem((outs, LANES), f32),
            vmem((channels, 2, 8, LANES), f32),
            vmem(square, f32), vmem((2, *square), f32), vmem((2, *square), f32),
            vmem((2, slabs, 8, LANES), f32), vmem((2, chains, reach, 8, LANES), f32),
            vmem((2, chains, 8, LANES), f32), vmem((2, arrivals, 8, LANES), f32),
            vmem((chans, 8, LANES), f32), vmem((chans - 1, 8, LANES), f32),
            vmem((2, slabs, 8, LANES), f32), vmem((8, LANES), f32),
            vmem((2, *square), f32), vmem((2, *square), f32),
            vmem((chans, 8, LANES), f32), vmem((4, 2, LANES), f32),
            vmem((3, 2, LANES), f32), vmem((slabs // 4 - 1, 2, LANES), f32),
            sems((7,)), sems((5,)), sems((5,)), sems((4, 3)), sems((2, chains)), sems((2,)),
            sems((2, chains)), sems((2,)), sems((2,)), sems((2,)), sems((2,)), sems((2,)),
        ],
        compiler_params=pltpu.CompilerParams(collective_id=0, has_side_effects=True, vmem_limit_bytes=40 << 20),
        name="fno_layer",
    )(
        *(
            pltpu.with_memory_space_constraint(a, pltpu.HBM)
            for a in (
                source_field.reshape(flat), cotangent.reshape(flat), w, skip_gain, channel_bias, limits, width_limit,
            )
        )
    )
    out, fgrad, sgrad, gate, bgrad = pl.pallas_call(
        functools.partial(finish, rows),
        out_shape=tuple(jax.ShapeDtypeStruct(*h) for h in held[:5]),
        in_specs=[vmem_spec] * len(held),
        out_specs=[hbm_spec] * 5,
        scratch_shapes=[vmem(flat, f32), pltpu.SemaphoreType.DMA((4,)), pltpu.SemaphoreType.DMA((4,))],
        compiler_params=pltpu.CompilerParams(vmem_limit_bytes=24 << 20),
        name="fno_finish",
    )(*found)
    sgrad = sgrad.reshape(channels, 16, 2, 2, outs).transpose(0, 4, 1, 2, 3)
    return (
        out.reshape(source_field.shape), fgrad.reshape(source_field.shape), sgrad,
        gate.reshape(channels), bgrad.reshape(channels),
    )


def solution(mesh):
    field = P(("member", "chan"), "slab", "mode")
    weight = P(("member", "chan"), None, "mode", None, "slab")
    channel = P(("member", "chan"))
    return jax.shard_map(
        local,
        mesh=mesh,
        in_specs=(field, field, weight, channel, channel, P("member", None), P("member")),
        out_specs=(field, field, weight, channel, channel),
        check_vma=False,
    )
```
